16 devices in a mesh: dp: 2 (over y, z), ep: 8 (over x, core).
Axes of the slice: x: 4, y: 2, z: 1, core: 2. Of those that a mesh axis runs over, the one named last changes fastest.
The devices are a block of a 4x4x8 slice.
Arguments:
- x_tokens: bfloat16 [1024, 1536], P(('dp', 'ep')), parts along dimension 0
- dy_tokens: bfloat16 [1024, 1536], P(('dp', 'ep')), parts along dimension 0
- expert_ids: int32 [1024, 8], P(('dp', 'ep')), parts along dimension 0
- gate_vals: float32 [1024, 8], P(('dp', 'ep')), parts along dimension 0
- slot_ids: int32 [1024, 8], P(('dp', 'ep')), parts along dimension 0
- w_gate: bfloat16 [40, 1536, 512], P('ep')
- w_down: bfloat16 [40, 512, 1536], P('ep')
- w_up: bfloat16 [40, 1536, 512], P('ep')
Outputs:
- output 1: bfloat16 [1024, 1536], P(('dp', 'ep')), parts along dimension 0
- output 2: float32 [80, 1536, 512], P(('dp', 'ep')), parts along dimension 0
- output 3: float32 [80, 512, 1536], P(('dp', 'ep')), parts along dimension 0
- output 4: float32 [80, 1536, 512], P(('dp', 'ep')), parts along dimension 0
There are 2 independent parts. The reference program is written for one: setup_inputs(seed, part) draws one part's arguments, and reference() takes and returns one part's arrays. A program takes and returns all parts, laid end to end along the dimension named above; an argument that names none is the same for every part.
All inputs are finite; a program needn't handle non-finite values.
Results may differ from the reference program's by a relative error of at most 0.0103792.
Values are sent between devices in bfloat16 or wider.
A program may use at most 768 MiB of HBM per device.

```python
import jax
import jax.numpy as jnp
from jax import lax

D = 1536
FF = 512
EXPERTS = 40
TOP = 8
GROUP = 8
TOK = 64
CAP = 24


def source_routing(src_key):
    key_base, key_offset, key_hot = jax.random.split(src_key, 3)
    stride = EXPERTS // TOP
    base_expert = jax.random.randint(key_base, (TOK,), 0, EXPERTS)
    offset = jax.random.randint(key_offset, (TOK, TOP), 0, stride)
    hot_expert = jax.random.randint(key_hot, (), 0, EXPERTS)
    forced = jnp.arange(TOK) < CAP
    base_expert = jnp.where(forced, hot_expert, base_expert)
    offset = jnp.where(forced[:, None] & (jnp.arange(TOP)[None, :] == 0), 0, offset)
    experts = (base_expert[:, None] + jnp.arange(TOP)[None, :] * stride + offset) % EXPERTS
    n_copy = TOK * TOP
    flat_exp = experts.reshape(n_copy)
    copy_ids = jnp.arange(n_copy)
    sort_order = jnp.argsort(flat_exp * n_copy + copy_ids)
    exp_counts = jnp.zeros((EXPERTS,), jnp.int32).at[flat_exp].add(1)
    exp_starts = jnp.cumsum(exp_counts) - exp_counts
    sorted_rank = copy_ids - exp_starts[flat_exp[sort_order]]
    copy_rank = jnp.zeros((n_copy,), jnp.int32).at[sort_order].set(sorted_rank)
    slots = jnp.where(copy_rank < CAP, copy_rank, -1)
    return experts.astype(jnp.int32), slots.reshape(TOK, TOP).astype(jnp.int32)


def setup_inputs(seed: int = 0, part: int = 0) -> dict:
    root_key = jax.random.key(seed)
    sub_keys = jax.random.split(root_key, 7)
    n_tok = GROUP * TOK
    x_tokens = jax.random.normal(jax.random.fold_in(sub_keys[0], part), (n_tok, D), jnp.float32).astype(jnp.bfloat16)
    dy_tokens = jax.random.normal(jax.random.fold_in(sub_keys[1], part), (n_tok, D), jnp.float32).astype(jnp.bfloat16)
    gate_vals = jax.random.uniform(jax.random.fold_in(sub_keys[2], part), (n_tok, TOP), jnp.float32, 0.3, 1.0)
    src_keys = jax.random.split(jax.random.fold_in(sub_keys[3], part), GROUP)
    expert_ids, slot_ids = jax.vmap(source_routing)(src_keys)
    w_gate = (jax.random.normal(sub_keys[4], (EXPERTS, D, FF), jnp.float32) * D ** -0.5).astype(jnp.bfloat16)
    w_down = (jax.random.normal(sub_keys[5], (EXPERTS, FF, D), jnp.float32) * FF ** -0.5).astype(jnp.bfloat16)
    w_up = (jax.random.normal(sub_keys[6], (EXPERTS, D, FF), jnp.float32) * D ** -0.5).astype(jnp.bfloat16)
    return {'x_tokens': x_tokens, 'dy_tokens': dy_tokens, 'expert_ids': expert_ids.reshape(n_tok, TOP), 'gate_vals': gate_vals, 'slot_ids': slot_ids.reshape(n_tok, TOP), 'w_gate': w_gate, 'w_down': w_down, 'w_up': w_up}


def expert_backward(operands):
    x_rows, dz_rows, w_gate, w_down, w_up = operands
    a_pre = jnp.dot(x_rows, w_gate, preferred_element_type=jnp.float32).astype(jnp.bfloat16).astype(jnp.float32)
    b_pre = jnp.dot(x_rows, w_up, preferred_element_type=jnp.float32).astype(jnp.bfloat16).astype(jnp.float32)
    sigma_a = jax.nn.sigmoid(a_pre)
    silu_a = a_pre * sigma_a
    hidden = (silu_a * b_pre).astype(jnp.bfloat16)
    d_hidden = jnp.dot(dz_rows, w_down.T, preferred_element_type=jnp.float32)
    d_gate = (d_hidden * b_pre * sigma_a * (1.0 + a_pre * (1.0 - sigma_a))).astype(jnp.bfloat16)
    d_up = (d_hidden * silu_a).astype(jnp.bfloat16)
    g_down = jnp.dot(hidden.T, dz_rows, preferred_element_type=jnp.float32)
    g_gate = jnp.dot(x_rows.T, d_gate, preferred_element_type=jnp.float32)
    g_up = jnp.dot(x_rows.T, d_up, preferred_element_type=jnp.float32)
    dx_rows = (jnp.dot(d_gate, w_gate.T, preferred_element_type=jnp.float32) + jnp.dot(d_up, w_up.T, preferred_element_type=jnp.float32)).astype(jnp.bfloat16)
    return dx_rows, g_gate, g_down, g_up


def reference(x_tokens, dy_tokens, expert_ids, gate_vals, slot_ids, w_gate, w_down, w_up):
    n_tok = GROUP * TOK
    n_rows = GROUP * CAP
    n_slot = EXPERTS * n_rows
    source = jnp.arange(n_tok) // TOK
    buf_index = jnp.where(slot_ids >= 0, expert_ids * n_rows + source[:, None] * CAP + slot_ids, n_slot)
    slot_copy = jnp.full((n_slot,), n_tok * TOP, jnp.int32).at[buf_index.reshape(n_tok * TOP)].set(jnp.arange(n_tok * TOP, dtype=jnp.int32), mode='drop')
    slot_tok = slot_copy // TOP
    x_buf = jnp.take(x_tokens, slot_tok, axis=0, mode='fill', fill_value=0).reshape(EXPERTS, n_rows, D)
    gate_slot = jnp.take(gate_vals.reshape(n_tok * TOP), slot_copy, mode='fill', fill_value=0)
    dy_slot = jnp.take(dy_tokens, slot_tok, axis=0, mode='fill', fill_value=0)
    dz_buf = (gate_slot[:, None] * dy_slot).astype(jnp.bfloat16).reshape(EXPERTS, n_rows, D)
    dx_buf, dw_gate, dw_down, dw_up = lax.map(expert_backward, (x_buf, dz_buf, w_gate, w_down, w_up))
    returned = jnp.take(dx_buf.reshape(n_slot, D), buf_index, axis=0, mode='fill', fill_value=0)
    dx_tokens = jnp.sum(returned.astype(jnp.float32), axis=1).astype(jnp.bfloat16)
    return (dx_tokens, dw_gate, dw_down, dw_up)
```

```python
import functools

import jax
import jax.numpy as jnp
from jax import lax
from jax.experimental import pallas as pl
from jax.experimental.pallas import tpu as pltpu
from jax.sharding import PartitionSpec as P

F32 = jnp.float32
BF16 = jnp.bfloat16
NT = (((1,), (1,)), ((), ()))
TN = (((0,), (0,)), ((), ()))
DY_Q = 3
DX_Q = 3
KEY_STRIDE = 256


def slot_capacity(tok_dev, top_k, n_exp):
    return ((3 * tok_dev * top_k) // (2 * n_exp) + 7) // 8 * 8


def exchange_kernel(
    n_dev, cap,
    x_hbm, dy_hbm, meta_hbm, w1_hbm, w3_hbm, w2_hbm,
    xbuf_o, dz_o, h_o, da_o, db_o, r1_o, l1_o, ra_o, lb_o, own_o,
    xg, dyg, mt, w1, w3, w2, xb, dz, hh, qq, uu, bb, dh, da, db, dxq,
    pm, pt, gm, part, sibr, sums,
    loc_sem, w_sem, out_sem, s_sem, send, recv,
):
    n_exp = w1_hbm.shape[0]
    tok, d = x_hbm.shape
    half = tok // 2
    n_chip = n_dev // 2
    rc_rows = 2 * cap
    used = n_exp * rc_rows
    me = lax.axis_index("ep")
    chip, core = me // 2, lax.rem(me, 2)
    right = lax.rem(chip + 1, n_chip) * 2 + core
    left = lax.rem(chip + n_chip - 1, n_chip) * 2 + core
    sib = chip * 2 + 1 - core

    counter = [0]

    def remote(src, dst, dev):
        i = counter[0]
        counter[0] += 1
        return pltpu.make_async_remote_copy(
            src_ref=src, dst_ref=dst, send_sem=send.at[i], recv_sem=recv.at[i],
            device_id={"ep": dev}, device_id_type=pl.DeviceIdType.MESH)

    started = []

    def go(copy):
        copy.start()
        started.append(copy)
        return copy

    loc = [
        pltpu.make_async_copy(meta_hbm, mt.at[0, 0], loc_sem.at[0]),
        pltpu.make_async_copy(x_hbm, xg.at[0, 0], loc_sem.at[1]),
        pltpu.make_async_copy(dy_hbm, dyg.at[0, 0], loc_sem.at[2]),
    ]
    for c in loc:
        c.start()
    wcopies = {}
    for k, (src, dst) in enumerate(((w1_hbm, w1), (w3_hbm, w3), (w2_hbm, w2))):
        for e in range(n_exp):
            wcopies[k, e] = pltpu.make_async_copy(src.at[e], dst.at[e], w_sem.at[k * n_exp + e])
    for e in range(n_exp):
        wcopies[0, e].start()
        wcopies[1, e].start()
    for e in range(n_exp):
        wcopies[2, e].start()

    barrier = pltpu.get_barrier_semaphore()
    for dev in (right, left, sib):
        pl.semaphore_signal(barrier, inc=1, device_id={"ep": dev}, device_id_type=pl.DeviceIdType.MESH)
    pl.semaphore_wait(barrier, 3)

    lo, hi = pl.ds(0, half), pl.ds(half, half)
    loc[0].wait()
    m_r = go(remote(mt.at[0, 0], mt.at[3, 0], right))
    m_l = go(remote(mt.at[0, 0], mt.at[1, 0], left))
    m_s = go(remote(mt.at[0, 0], mt.at[0, 1], sib))
    loc[1].wait()
    xa_r = go(remote(xg.at[0, 0, lo], xg.at[3, 0, lo], right))
    xb_l = go(remote(xg.at[0, 0, hi], xg.at[1, 0, hi], left))
    xb_r = go(remote(xg.at[0, 0, hi], xg.at[3, 0, hi], right))
    xa_l = go(remote(xg.at[0, 0, lo], xg.at[1, 0, lo], left))
    x_s = go(remote(xg.at[0, 0], xg.at[0, 1], sib))
    m_r.wait_recv()
    m_rr = go(remote(mt.at[3, 0], mt.at[2, 0], right))
    m_s3 = go(remote(mt.at[3, 0], mt.at[3, 1], sib))
    m_l.wait_recv()
    m_s1 = go(remote(mt.at[1, 0], mt.at[1, 1], sib))
    xa_r.wait_recv()
    xa_rr = go(remote(xg.at[3, 0, lo], xg.at[2, 0, lo], right))
    xb_l.wait_recv()
    xb_ll = go(remote(xg.at[1, 0, hi], xg.at[2, 0, hi], left))

    loc[2].wait()
    qd = d // DY_Q
    dcol = [pl.ds(q * qd, qd) for q in range(DY_Q)]
    dy = {}

    def dy_own(q):
        c = dcol[q]
        dy["ar", q] = go(remote(dyg.at[0, 0, lo, c], dyg.at[3, 0, lo, c], right))
        dy["bl", q] = go(remote(dyg.at[0, 0, hi, c], dyg.at[1, 0, hi, c], left))
        dy["br", q] = go(remote(dyg.at[0, 0, hi, c], dyg.at[3, 0, hi, c], right))
        dy["al", q] = go(remote(dyg.at[0, 0, lo, c], dyg.at[1, 0, lo, c], left))
        dy["s0", q] = go(remote(dyg.at[0, 0, :, c], dyg.at[0, 1, :, c], sib))

    def dy_relay(q):
        c = dcol[q]
        dy["ar", q].wait_recv()
        dy["arr", q] = go(remote(dyg.at[3, 0, lo, c], dyg.at[2, 0, lo, c], right))
        dy["bl", q].wait_recv()
        dy["bll", q] = go(remote(dyg.at[1, 0, hi, c], dyg.at[2, 0, hi, c], left))
        dy["br", q].wait_recv()
        dy["s3", q] = go(remote(dyg.at[3, 0, :, c], dyg.at[3, 1, :, c], sib))
        dy["al", q].wait_recv()
        dy["s1", q] = go(remote(dyg.at[1, 0, :, c], dyg.at[1, 1, :, c], sib))

    def dy_far(q):
        c = dcol[q]
        dy["arr", q].wait_recv()
        dy["bll", q].wait_recv()
        dy["s2", q] = go(remote(dyg.at[2, 0, :, c], dyg.at[2, 1, :, c], sib))

    dy_own(0)
    dy_own(1)

    rows_i = lax.broadcasted_iota(jnp.int32, (KEY_STRIDE, 2 * tok), 0)
    lane_i = lax.broadcasted_iota(jnp.int32, (16, 2 * tok), 1)
    row_key = (rows_i + me * KEY_STRIDE).astype(F32)

    def build(s):
        m0, m1 = mt[s, 0], mt[s, 1]
        first = lane_i < tok
        keys = jnp.where(first, m0, m1 + float(cap))
        gates = jnp.where(first, m0, m1)
        ones = jnp.zeros((KEY_STRIDE, 2 * tok), F32)
        gmat = jnp.zeros((KEY_STRIDE, 2 * tok), F32)
        for j in range(8):
            hit = row_key == keys[j:j + 1, :]
            ones = jnp.where(hit, 1.0, ones)
            gmat = jnp.where(hit, gates[8 + j:9 + j, :], gmat)
        pm[s] = ones.astype(BF16)
        pt[s] = jnp.transpose(ones).astype(BF16)
        gm[s] = jnp.sum(gmat, axis=1, keepdims=True)

    m_s.wait_recv()
    build(0)
    m_s3.wait_recv()
    build(3)
    m_s1.wait_recv()
    build(1)
    m_rr.wait_recv()
    m_s2 = go(remote(mt.at[2, 0], mt.at[2, 1], sib))

    def gather_x(s):
        src = xg[s].reshape(2 * tok, d)
        rows = jnp.dot(pm[s, :used, :], src, preferred_element_type=F32).astype(BF16)
        for e in range(n_exp):
            xb[e, s * rc_rows:(s + 1) * rc_rows, :] = rows[e * rc_rows:(e + 1) * rc_rows, :]

    xb_r.wait_recv()
    x_s3 = go(remote(xg.at[3, 0], xg.at[3, 1], sib))
    xa_l.wait_recv()
    x_s1 = go(remote(xg.at[1, 0], xg.at[1, 1], sib))
    x_s.wait_recv()
    gather_x(0)
    x_s3.wait_recv()
    gather_x(3)
    m_s2.wait_recv()
    build(2)
    x_s1.wait_recv()
    gather_x(1)
    xa_rr.wait_recv()
    xb_ll.wait_recv()
    x_s2 = go(remote(xg.at[2, 0], xg.at[2, 1], sib))
    x_s2.wait_recv()
    gather_x(2)

    outs = []

    def put(src, dst):
        i = len(outs)
        c = pltpu.make_async_copy(src, dst, out_sem.at[i])
        c.start()
        outs.append(c)

    def up(e):
        wcopies[0, e].wait()
        wcopies[1, e].wait()
        x = xb[e]
        a16 = jnp.dot(x, w1[e], preferred_element_type=F32).astype(BF16)
        b16 = jnp.dot(x, w3[e], preferred_element_type=F32).astype(BF16)
        a = a16.astype(F32)
        b = b16.astype(F32)
        sg = jax.nn.sigmoid(a)
        silu = a * sg
        hh[e] = (silu * b).astype(BF16)
        uu[e] = silu
        qq[e] = sg * (1.0 + a * (1.0 - sg))
        bb[e] = b16

    put(xb, xbuf_o)
    for e in range(n_exp):
        up(e)
        if e == 0:
            dy_relay(0)
            dy_own(2)
        if e == 2:
            dy_relay(1)
    put(hh, h_o)
    dy_far(0)

    def gather_dy(q):
        c = slice(q * qd, (q + 1) * qd)
        for s, key in ((0, "s0"), (3, "s3"), (1, "s1"), (2, "s2")):
            dy[key, q].wait_recv()
            src = dyg[s, :, :, c].reshape(2 * tok, qd)
            rows = jnp.dot(pm[s, :used, :], src, preferred_element_type=F32)
            rows = (rows * gm[s, :used, :]).astype(BF16)
            for e in range(n_exp):
                dz[e, s * rc_rows:(s + 1) * rc_rows, c] = rows[e * rc_rows:(e + 1) * rc_rows, :]

    def down(e, q):
        c = slice(q * qd, (q + 1) * qd)
        if q == 0:
            wcopies[2, e].wait()
        val = lax.dot_general(dz[e, :, c], w2[e, :, c], NT, preferred_element_type=F32)
        if q > 0:
            val = val + dh[e]
        if q < DY_Q - 1:
            dh[e] = val
        else:
            da[e] = (val * bb[e].astype(F32) * qq[e]).astype(BF16)
            db[e] = (val * uu[e]).astype(BF16)

    for q in range(DY_Q):
        if q == 0:
            dy_relay(2)
        if q == 1:
            dy_far(1)
        if q == 2:
            dy_far(2)
        gather_dy(q)
        for e in range(n_exp):
            down(e, q)
    put(dz, dz_o)
    put(da, da_o)
    put(db, db_o)

    qx = d // DX_Q
    sib_copies = []

    def dx_block(q):
        c = slice(q * qx, (q + 1) * qx)
        for e in range(n_exp):
            v = lax.dot_general(da[e], w1[e, c, :], NT, preferred_element_type=F32)
            v = v + lax.dot_general(db[e], w3[e, c, :], NT, preferred_element_type=F32)
            dxq[e] = v.astype(BF16)
        for s in range(n_chip):
            rows = dxq[:, s * rc_rows:(s + 1) * rc_rows, :].reshape(used, qx)
            part[q, s] = jnp.dot(pt[s, :, :used], rows, preferred_element_type=F32).reshape(2, tok, qx)
        sib_copies.append(go(remote(part.at[q, :, 1], sibr.at[q], sib)))

    def finish(q):
        c = slice(q * qx, (q + 1) * qx)
        sib_copies[q].wait_recv()
        for s in range(n_chip):
            sums[s, :, c] = part[q, s, 0] + sibr[q, s]

    for q in range(DX_Q):
        dx_block(q)
        if q > 0:
            finish(q - 1)
    finish(DX_Q - 1)

    put(sums.at[2, lo], r1_o.at[lo])
    put(sums.at[1, hi], r1_o.at[hi])
    put(sums.at[3, lo], l1_o.at[lo])
    put(sums.at[2, hi], l1_o.at[hi])
    put(sums.at[1, lo], ra_o)
    put(sums.at[3, hi], lb_o)
    put(sums.at[0], own_o)
    for c in outs:
        c.wait()
    for c in started:
        c.wait_send()


def run_exchange(x, dy, meta, w1, w3, w2, n_dev, cap):
    n_exp, d, f = w1.shape
    tok = x.shape[0]
    half = tok // 2
    n_chip = n_dev // 2
    rows = n_dev * cap
    used = n_exp * 2 * cap
    qx = d // DX_Q
    any_spec = pl.BlockSpec(memory_space=pl.ANY)
    sds = jax.ShapeDtypeStruct
    outs = (
        sds((n_exp, rows, d), BF16), sds((n_exp, rows, d), BF16),
        sds((n_exp, rows, f), BF16), sds((n_exp, rows, f), BF16), sds((n_exp, rows, f), BF16),
        sds((tok, d), F32), sds((tok, d), F32), sds((half, d), F32), sds((half, d), F32), sds((tok, d), F32),
    )
    n_copies = 80
    scratch = [
        pltpu.VMEM((n_chip, 2, tok, d), BF16),
        pltpu.VMEM((n_chip, 2, tok, d), BF16),
        pltpu.VMEM((n_chip, 2, 16, 2 * tok), F32),
        pltpu.VMEM((n_exp, d, f), BF16),
        pltpu.VMEM((n_exp, d, f), BF16),
        pltpu.VMEM((n_exp, f, d), BF16),
        pltpu.VMEM((n_exp, rows, d), BF16),
        pltpu.VMEM((n_exp, rows, d), BF16),
        pltpu.VMEM((n_exp, rows, f), BF16),
        pltpu.VMEM((n_exp, rows, f), F32),
        pltpu.VMEM((n_exp, rows, f), F32),
        pltpu.VMEM((n_exp, rows, f), BF16),
        pltpu.VMEM((n_exp, rows, f), F32),
        pltpu.VMEM((n_exp, rows, f), BF16),
        pltpu.VMEM((n_exp, rows, f), BF16),
        pltpu.VMEM((n_exp, rows, qx), BF16),
        pltpu.VMEM((n_chip, KEY_STRIDE, 2 * tok), BF16),
        pltpu.VMEM((n_chip, 2 * tok, KEY_STRIDE), BF16),
        pltpu.VMEM((n_chip, KEY_STRIDE, 1), F32),
        pltpu.VMEM((DX_Q, n_chip, 2, tok, qx), F32),
        pltpu.VMEM((DX_Q, n_chip, tok, qx), F32),
        pltpu.VMEM((n_chip, tok, d), F32),
        pltpu.SemaphoreType.DMA((3,)),
        pltpu.SemaphoreType.DMA((3 * n_exp,)),
        pltpu.SemaphoreType.DMA((16,)),
        pltpu.SemaphoreType.DMA((1,)),
        pltpu.SemaphoreType.DMA((n_copies,)),
        pltpu.SemaphoreType.DMA((n_copies,)),
    ]
    return pl.pallas_call(
        functools.partial(exchange_kernel, n_dev, cap),
        out_shape=outs,
        in_specs=[any_spec] * 6,
        out_specs=(any_spec,) * len(outs),
        scratch_shapes=scratch,
        compiler_params=pltpu.CompilerParams(
            collective_id=0, has_side_effects=True, vmem_limit_bytes=64_000_000),
        name="exchange",
    )(x, dy, meta, w1, w3, w2)


def grad_in_kernel(x_ref, da_ref, db_ref, g1_ref, g3_ref):
    x = x_ref[0]
    g1_ref[0] = lax.dot_general(x, da_ref[0], TN, preferred_element_type=F32)
    g3_ref[0] = lax.dot_general(x, db_ref[0], TN, preferred_element_type=F32)


def grad_in(xb, da, db, blk=512):
    n_exp, rows, d = xb.shape
    f = da.shape[2]
    row_spec = pl.BlockSpec((1, rows, f), lambda e, k: (e, 0, 0))
    out_spec = pl.BlockSpec((1, blk, f), lambda e, k: (e, k, 0))
    out = jax.ShapeDtypeStruct((n_exp, d, f), F32)
    return pl.pallas_call(
        grad_in_kernel,
        grid=(n_exp, d // blk),
        out_shape=(out, out),
        in_specs=[pl.BlockSpec((1, rows, blk), lambda e, k: (e, 0, k)), row_spec, row_spec],
        out_specs=(out_spec, out_spec),
        cost_estimate=pl.CostEstimate(flops=4 * n_exp * rows * d * f, bytes_accessed=8 * n_exp * d * f, transcendentals=0),
        name="grad_in",
    )(xb, da, db)


def grad_out_kernel(h_ref, dz_ref, g_ref):
    g_ref[0] = lax.dot_general(h_ref[0], dz_ref[0], TN, preferred_element_type=F32)


def grad_out(h, dz, blk=256):
    n_exp, rows, f = h.shape
    d = dz.shape[2]
    return pl.pallas_call(
        grad_out_kernel,
        grid=(n_exp, f // blk),
        out_shape=jax.ShapeDtypeStruct((n_exp, f, d), F32),
        in_specs=[pl.BlockSpec((1, rows, blk), lambda e, k: (e, 0, k)), pl.BlockSpec((1, rows, d), lambda e, k: (e, 0, 0))],
        out_specs=pl.BlockSpec((1, blk, d), lambda e, k: (e, k, 0)),
        cost_estimate=pl.CostEstimate(flops=2 * n_exp * rows * d * f, bytes_accessed=4 * n_exp * d * f, transcendentals=0),
        name="grad_out",
    )(h, dz)


def solution(mesh):
    n_dev = mesh.shape["ep"]
    n_chip = n_dev // 2

    def local_step(x_loc, dy_loc, ids_loc, gate_loc, slot_loc, w_gate, w_down, w_up):
        tok, top_k = ids_loc.shape
        n_local = w_gate.shape[0]
        cap = slot_capacity(tok, top_k, n_local * n_dev)
        half = tok // 2
        keys = (ids_loc // n_local) * KEY_STRIDE + (ids_loc % n_local) * (2 * cap) + slot_loc
        keys = jnp.where(slot_loc >= 0, keys, -1000).astype(F32)
        meta = jnp.concatenate([keys.T, gate_loc.T], axis=0)
        meta = jnp.concatenate([meta, meta], axis=1)
        xb, dz, h, da, db, r1, l1, ra, lb, own = run_exchange(
            x_loc, dy_loc, meta, w_gate, w_up, w_down, n_dev, cap)
        to_right = [(c * 2 + k, (c + 1) % n_chip * 2 + k) for c in range(n_chip) for k in range(2)]
        to_left = [(b, a) for a, b in to_right]
        r1 = lax.ppermute(r1, "ep", to_right)
        l1 = lax.ppermute(l1, "ep", to_left)
        g_gate, g_up = grad_in(xb, da, db)
        g_gate, g_up, r1, l1 = lax.optimization_barrier((g_gate, g_up, r1, l1))
        r2 = lax.ppermute(ra + r1[:half], "ep", to_right)
        l2 = lax.ppermute(lb + l1[half:], "ep", to_left)
        g_down = grad_out(h, dz)
        dx_lo = own[:half] + l1[:half] + r2
        dx_hi = own[half:] + r1[half:] + l2
        dx = jnp.concatenate([dx_lo, dx_hi], axis=0).astype(BF16)
        return dx, g_gate, g_down, g_up

    tok_spec = P(("dp", "ep"), None)
    w_spec = P("ep", None, None)
    grad_spec = P(("dp", "ep"), None, None)
    return jax.shard_map(
        local_step, mesh=mesh,
        in_specs=(tok_spec,) * 5 + (w_spec,) * 3,
        out_specs=(tok_spec, grad_spec, grad_spec, grad_spec),
        check_vma=False)
```

```python
import functools

import jax
import jax.numpy as jnp
from jax import lax
from jax.experimental import pallas as pl
from jax.experimental.pallas import tpu as pltpu
from jax.sharding import PartitionSpec as P

F32 = jnp.float32
BF16 = jnp.bfloat16
NT = (((1,), (1,)), ((), ()))
TN = (((0,), (0,)), ((), ()))
DY_Q = 3
DX_Q = 3
KEY_STRIDE = 256
N_COPIES = 36
OUT_TYPE = pltpu.VMEM


def slot_capacity(tok_dev, top_k, n_exp):
    return ((3 * tok_dev * top_k) // (2 * n_exp) + 7) // 8 * 8


def exchange_kernel(
    n_dev, cap,
    x_hbm, dy_hbm, ids_hbm, slot_hbm, gate_hbm, w1_hbm, w3_hbm, w2_hbm,
    xb, dz, hh, da, db, r1, l1, ra, lb, own,
    xg, dyg, ids, slots, gates_v, mt, w1, w3, w2, qq, uu, bb, dh, dxq,
    pm, pt, gm, part, sibr,
    loc_sem, w_sem, send, recv,
):
    n_exp = w1_hbm.shape[0]
    tok, d = x_hbm.shape
    half = tok // 2
    n_chip = n_dev // 2
    rc_rows = 2 * cap
    used = n_exp * rc_rows
    me = lax.axis_index("ep")
    chip, core = me // 2, lax.rem(me, 2)
    right = lax.rem(chip + 1, n_chip) * 2 + core
    left = lax.rem(chip + n_chip - 1, n_chip) * 2 + core
    sib = chip * 2 + 1 - core

    counter = [0]

    def remote(src, dst, dev):
        i = counter[0]
        counter[0] += 1
        return pltpu.make_async_remote_copy(
            src_ref=src, dst_ref=dst, send_sem=send.at[i], recv_sem=recv.at[i],
            device_id={"ep": dev}, device_id_type=pl.DeviceIdType.MESH)

    started = []

    def go(copy):
        copy.start()
        started.append(copy)
        return copy

    barrier = pltpu.get_barrier_semaphore()
    for dev in (right, left, sib):
        pl.semaphore_signal(barrier, inc=1, device_id={"ep": dev}, device_id_type=pl.DeviceIdType.MESH)

    loc = [
        pltpu.make_async_copy(src, dst, loc_sem.at[i])
        for i, (src, dst) in enumerate((
            (ids_hbm, ids), (slot_hbm, slots), (gate_hbm, gates_v),
            (x_hbm, xg.at[0, 0]), (dy_hbm, dyg.at[0, 0])))
    ]
    for c in loc:
        c.start()
    wcopies = {}
    for k, (src, dst) in enumerate(((w1_hbm, w1), (w3_hbm, w3), (w2_hbm, w2))):
        for e in range(n_exp):
            wcopies[k, e] = pltpu.make_async_copy(src.at[e], dst.at[e], w_sem.at[k * n_exp + e])

    with jax.named_scope("head_keys"):
        for c in loc[:3]:
            c.wait()
        expert, slot = ids[...].astype(F32), slots[...].astype(F32)
        owner = jnp.floor((expert + 0.5) / float(n_exp))
        keys = owner * float(KEY_STRIDE) + (expert - owner * n_exp) * float(rc_rows) + slot
        keys = jnp.where(slot >= 0.0, keys, -1000.0)
        for i in range(2):
            mt[0, 0, :8, i * tok:(i + 1) * tok] = keys
            mt[0, 0, 8:, i * tok:(i + 1) * tok] = gates_v[...]

    with jax.named_scope("head_barrier"):
        pl.semaphore_wait(barrier, 3)

    rows_i = lax.broadcasted_iota(jnp.int32, (KEY_STRIDE, 2 * tok), 0)
    lane_i = lax.broadcasted_iota(jnp.int32, (16, 2 * tok), 1)
    row_key = (rows_i + me * KEY_STRIDE).astype(F32)

    def build(s):
        m0, m1 = mt[s, 0], mt[s, 1]
        first = lane_i < tok
        keys = jnp.where(first, m0, m1 + float(cap))
        gates = jnp.where(first, m0, m1)
        ones = jnp.zeros((KEY_STRIDE, 2 * tok), F32)
        gmat = jnp.zeros((KEY_STRIDE, 2 * tok), F32)
        for j in range(8):
            hit = row_key == keys[j:j + 1, :]
            ones = jnp.where(hit, 1.0, ones)
            gmat = jnp.where(hit, gates[8 + j:9 + j, :], gmat)
        pm[s] = ones.astype(BF16)
        pt[s] = jnp.transpose(ones).astype(BF16)
        gm[s] = jnp.sum(gmat, axis=1, keepdims=True)

    def gather_x(s):
        src = xg[s].reshape(2 * tok, d)
        rows = jnp.dot(pm[s, :used, :], src, preferred_element_type=F32).astype(BF16)
        for e in range(n_exp):
            xb[e, s * rc_rows:(s + 1) * rc_rows, :] = rows[e * rc_rows:(e + 1) * rc_rows, :]

    def gather_dy(s, c):
        src = dyg[s, :, :, c].reshape(2 * tok, c.stop - c.start)
        rows = jnp.dot(pm[s, :used, :], src, preferred_element_type=F32)
        rows = (rows * gm[s, :used, :]).astype(BF16)
        for e in range(n_exp):
            dz[e, s * rc_rows:(s + 1) * rc_rows, c] = rows[e * rc_rows:(e + 1) * rc_rows, :]

    def up(e):
        wcopies[0, e].wait()
        wcopies[1, e].wait()
        x = xb[e]
        a16 = jnp.dot(x, w1[e], preferred_element_type=F32).astype(BF16)
        b16 = jnp.dot(x, w3[e], preferred_element_type=F32).astype(BF16)
        a = a16.astype(F32)
        b = b16.astype(F32)
        sg = jax.nn.sigmoid(a)
        silu = a * sg
        hh[e] = (silu * b).astype(BF16)
        uu[e] = silu
        qq[e] = sg * (1.0 + a * (1.0 - sg))
        bb[e] = b16

    lo, hi = pl.ds(0, half), pl.ds(half, half)
    qd = d // DY_Q
    dcol = [slice(q * qd, (q + 1) * qd) for q in range(DY_Q)]
    full = slice(0, d)

    def far_cols(q):
        return pl.ds(q * qd, qd)

    m_r = go(remote(mt.at[0, 0], mt.at[3, 0], right))
    m_l = go(remote(mt.at[0, 0], mt.at[1, 0], left))
    m_s = go(remote(mt.at[0, 0], mt.at[0, 1], sib))
    loc[3].wait()
    xa_r = go(remote(xg.at[0, 0, lo], xg.at[3, 0, lo], right))
    xb_l = go(remote(xg.at[0, 0, hi], xg.at[1, 0, hi], left))
    xb_r = go(remote(xg.at[0, 0, hi], xg.at[3, 0, hi], right))
    xa_l = go(remote(xg.at[0, 0, lo], xg.at[1, 0, lo], left))
    x_s = go(remote(xg.at[0, 0], xg.at[0, 1], sib))
    loc[4].wait()
    y_s = go(remote(dyg.at[0, 0], dyg.at[0, 1], sib))
    for e in range(n_exp):
        wcopies[0, e].start()
        wcopies[1, e].start()
    for e in range(n_exp):
        wcopies[2, e].start()
    with jax.named_scope("own_rows"):
        m_s.wait_recv()
        build(0)
        m_r.wait_recv()
        m_rr = go(remote(mt.at[3, 0], mt.at[2, 0], right))
        m_s3 = go(remote(mt.at[3, 0], mt.at[3, 1], sib))
        m_l.wait_recv()
        m_s1 = go(remote(mt.at[1, 0], mt.at[1, 1], sib))
        x_s.wait_recv()
        gather_x(0)
    with jax.named_scope("x_relay"):
        xa_r.wait_recv()
        xa_rr = go(remote(xg.at[3, 0, lo], xg.at[2, 0, lo], right))
        xb_l.wait_recv()
        xb_ll = go(remote(xg.at[1, 0, hi], xg.at[2, 0, hi], left))
        ya_r = go(remote(dyg.at[0, 0, lo], dyg.at[3, 0, lo], right))
        yb_l = go(remote(dyg.at[0, 0, hi], dyg.at[1, 0, hi], left))
        yb_r = go(remote(dyg.at[0, 0, hi], dyg.at[3, 0, hi], right))
        ya_l = go(remote(dyg.at[0, 0, lo], dyg.at[1, 0, lo], left))
    with jax.named_scope("build31"):
        m_s3.wait_recv()
        build(3)
        m_s1.wait_recv()
        build(1)
    with jax.named_scope("x_near"):
        xb_r.wait_recv()
        x_s3 = go(remote(xg.at[3, 0], xg.at[3, 1], sib))
        xa_l.wait_recv()
        x_s1 = go(remote(xg.at[1, 0], xg.at[1, 1], sib))
        m_rr.wait_recv()
        m_s2 = go(remote(mt.at[2, 0], mt.at[2, 1], sib))
        y_s.wait_recv()
        gather_dy(0, full)
        x_s3.wait_recv()
        gather_x(3)
        x_s1.wait_recv()
        gather_x(1)
    with jax.named_scope("x_far"):
        m_s2.wait_recv()
        build(2)
        xa_rr.wait_recv()
        xb_ll.wait_recv()
        x_s2 = go(remote(xg.at[2, 0], xg.at[2, 1], sib))
        x_s2.wait_recv()
        gather_x(2)
    with jax.named_scope("up0"):
        up(0)
    with jax.named_scope("y_relay"):
        ya_r.wait_recv()
        yb_l.wait_recv()
        yfar = []
        for q in range(DY_Q):
            c = far_cols(q)
            yfar.append((go(remote(dyg.at[3, 0, lo, c], dyg.at[2, 0, lo, c], right)),
                         go(remote(dyg.at[1, 0, hi, c], dyg.at[2, 0, hi, c], left))))
    with jax.named_scope("up12"):
        up(1)
        up(2)
    with jax.named_scope("y_near_fwd"):
        yb_r.wait_recv()
        y_s3 = go(remote(dyg.at[3, 0], dyg.at[3, 1], sib))
        ya_l.wait_recv()
        y_s1 = go(remote(dyg.at[1, 0], dyg.at[1, 1], sib))
    with jax.named_scope("up34"):
        for e in range(3, n_exp):
            up(e)

    y_s2 = []

    def y_far_fwd(q):
        c = far_cols(q)
        for copy in yfar[q]:
            copy.wait_recv()
        y_s2.append(go(remote(dyg.at[2, 0, :, c], dyg.at[2, 1, :, c], sib)))

    with jax.named_scope("y_near"):
        y_far_fwd(0)
        y_s3.wait_recv()
        gather_dy(3, full)
        y_s1.wait_recv()
        gather_dy(1, full)

    def down(e, q):
        c = dcol[q]
        if q == 0:
            wcopies[2, e].wait()
        val = lax.dot_general(dz[e, :, c], w2[e, :, c], NT, preferred_element_type=F32)
        if q > 0:
            val = val + dh[e]
        if q < DY_Q - 1:
            dh[e] = val
        else:
            da[e] = (val * bb[e].astype(F32) * qq[e]).astype(BF16)
            db[e] = (val * uu[e]).astype(BF16)

    for q in range(DY_Q):
        with jax.named_scope(f"y_far{q}"):
            if q + 1 < DY_Q:
                y_far_fwd(q + 1)
            y_s2[q].wait_recv()
            gather_dy(2, dcol[q])
        with jax.named_scope(f"down{q}"):
            for e in range(n_exp):
                down(e, q)

    qx = d // DX_Q
    sib_copies = []

    def dx_block(q):
        c = slice(q * qx, (q + 1) * qx)
        for e in range(n_exp):
            v = lax.dot_general(da[e], w1[e, c, :], NT, preferred_element_type=F32)
            v = v + lax.dot_general(db[e], w3[e, c, :], NT, preferred_element_type=F32)
            dxq[e] = v.astype(BF16)
        for s in range(n_chip):
            rows = dxq[:, s * rc_rows:(s + 1) * rc_rows, :].reshape(used, qx)
            part[q, s] = jnp.dot(pt[s, :, :used], rows, preferred_element_type=F32).reshape(2, tok, qx)
        sib_copies.append(go(remote(part.at[q, :, 1], sibr.at[q], sib)))

    def finish(q):
        c = slice(q * qx, (q + 1) * qx)
        sib_copies[q].wait_recv()

        def total(s, rs):
            return part[q, s, 0, rs] + sibr[q, s, rs]

        a, b = slice(0, half), slice(half, tok)
        r1[a, c] = total(2, a)
        r1[b, c] = total(1, b)
        l1[a, c] = total(3, a)
        l1[b, c] = total(2, b)
        ra[:, c] = total(1, a)
        lb[:, c] = total(3, b)
        own[:, c] = part[q, 0, 0] + sibr[q, 0]

    for q in range(DX_Q):
        with jax.named_scope(f"dx{q}"):
            dx_block(q)
        if q > 0:
            with jax.named_scope(f"finish{q - 1}"):
                finish(q - 1)
    with jax.named_scope(f"finish{DX_Q - 1}"):
        finish(DX_Q - 1)

    with jax.named_scope("send_wait"):
        for c in started:
            c.wait_send()
    assert counter[0] == N_COPIES


def run_exchange(x, dy, ids, slots, gates, w1, w3, w2, n_dev, cap):
    n_exp, d, f = w1.shape
    tok = x.shape[0]
    half = tok // 2
    n_chip = n_dev // 2
    rows = n_dev * cap
    used = n_exp * 2 * cap
    qx = d // DX_Q
    any_spec = pl.BlockSpec(memory_space=pl.ANY)
    vmem_spec = pl.BlockSpec(memory_space=pltpu.VMEM)
    sds = OUT_TYPE
    outs = (
        sds((n_exp, rows, d), BF16), sds((n_exp, rows, d), BF16),
        sds((n_exp, rows, f), BF16), sds((n_exp, rows, f), BF16), sds((n_exp, rows, f), BF16),
        sds((tok, d), F32), sds((tok, d), F32), sds((half, d), F32), sds((half, d), F32), sds((tok, d), F32),
    )
    scratch = [
        pltpu.VMEM((n_chip, 2, tok, d), BF16),
        pltpu.VMEM((n_chip, 2, tok, d), BF16),
        pltpu.VMEM(ids.shape, jnp.int32),
        pltpu.VMEM(ids.shape, jnp.int32),
        pltpu.VMEM(ids.shape, F32),
        pltpu.VMEM((n_chip, 2, 16, 2 * tok), F32),
        pltpu.VMEM((n_exp, d, f), BF16),
        pltpu.VMEM((n_exp, d, f), BF16),
        pltpu.VMEM((n_exp, f, d), BF16),
        pltpu.VMEM((n_exp, rows, f), F32),
        pltpu.VMEM((n_exp, rows, f), F32),
        pltpu.VMEM((n_exp, rows, f), BF16),
        pltpu.VMEM((n_exp, rows, f), F32),
        pltpu.VMEM((n_exp, rows, qx), BF16),
        pltpu.VMEM((n_chip, KEY_STRIDE, 2 * tok), BF16),
        pltpu.VMEM((n_chip, 2 * tok, KEY_STRIDE), BF16),
        pltpu.VMEM((n_chip, KEY_STRIDE, 1), F32),
        pltpu.VMEM((DX_Q, n_chip, 2, tok, qx), F32),
        pltpu.VMEM((DX_Q, n_chip, tok, qx), F32),
        pltpu.SemaphoreType.DMA((5,)),
        pltpu.SemaphoreType.DMA((3 * n_exp,)),
        pltpu.SemaphoreType.DMA((N_COPIES,)),
        pltpu.SemaphoreType.DMA((N_COPIES,)),
    ]
    return pl.pallas_call(
        functools.partial(exchange_kernel, n_dev, cap),
        out_shape=outs,
        in_specs=[any_spec] * 8,
        out_specs=(vmem_spec,) * len(outs),
        scratch_shapes=scratch,
        compiler_params=pltpu.CompilerParams(
            collective_id=0, has_side_effects=True, vmem_limit_bytes=54_000_000),
        name="exchange",
    )(x, dy, ids, slots, gates, w1, w3, w2)


def grad_in_kernel(blk, x, da, db, g1_hbm, g3_hbm, g1, g3, sem):
    n_exp, rows, d = x.shape
    n_blk = d // blk

    def store(e, k):
        rs = pl.ds(k * blk, blk)
        return [pltpu.make_async_copy(src.at[e, rs], dst.at[e, rs], sem.at[o, e, k])
                for o, (src, dst) in enumerate(((g1, g1_hbm), (g3, g3_hbm)))]

    def step(e, carry):
        for k in range(n_blk):
            rs = slice(k * blk, (k + 1) * blk)
            xt = x[e, :, rs]
            g1[e, rs, :] = lax.dot_general(xt, da[e], TN, preferred_element_type=F32)
            g3[e, rs, :] = lax.dot_general(xt, db[e], TN, preferred_element_type=F32)
            for c in store(e, k):
                c.start()
        return carry

    lax.fori_loop(0, n_exp, step, 0)

    def drain(e, carry):
        for k in range(n_blk):
            for c in store(e, k):
                c.wait()
        return carry

    lax.fori_loop(0, n_exp, drain, 0)


def grad_in(xb, da, db, blk=512):
    n_exp, rows, d = xb.shape
    f = da.shape[2]
    any_spec = pl.BlockSpec(memory_space=pl.ANY)
    out = jax.ShapeDtypeStruct((n_exp, d, f), F32)
    return pl.pallas_call(
        functools.partial(grad_in_kernel, blk),
        out_shape=(out, out),
        in_specs=[pl.BlockSpec(memory_space=pltpu.VMEM)] * 3,
        out_specs=(any_spec, any_spec),
        scratch_shapes=[
            pltpu.VMEM(out.shape, F32), pltpu.VMEM(out.shape, F32),
            pltpu.SemaphoreType.DMA((2, n_exp, d // blk))],
        compiler_params=pltpu.CompilerParams(vmem_limit_bytes=40_000_000),
        cost_estimate=pl.CostEstimate(flops=4 * n_exp * rows * d * f, bytes_accessed=8 * n_exp * d * f, transcendentals=0),
        name="grad_in",
    )(xb, da, db)


def grad_out_kernel(blk, h, dz, g_hbm, g, sem):
    n_exp, rows, f = h.shape
    n_blk = f // blk

    def store(e, k):
        rs = pl.ds(k * blk, blk)
        return pltpu.make_async_copy(g.at[e, rs], g_hbm.at[e, rs], sem.at[e, k])

    def step(e, carry):
        for k in range(n_blk):
            rs = slice(k * blk, (k + 1) * blk)
            g[e, rs, :] = lax.dot_general(h[e, :, rs], dz[e], TN, preferred_element_type=F32)
            store(e, k).start()
        return carry

    lax.fori_loop(0, n_exp, step, 0)

    def drain(e, carry):
        for k in range(n_blk):
            store(e, k).wait()
        return carry

    lax.fori_loop(0, n_exp, drain, 0)


def grad_out(h, dz, blk=256):
    n_exp, rows, f = h.shape
    d = dz.shape[2]
    out = jax.ShapeDtypeStruct((n_exp, f, d), F32)
    return pl.pallas_call(
        functools.partial(grad_out_kernel, blk),
        out_shape=out,
        in_specs=[pl.BlockSpec(memory_space=pltpu.VMEM)] * 2,
        out_specs=pl.BlockSpec(memory_space=pl.ANY),
        scratch_shapes=[pltpu.VMEM(out.shape, F32), pltpu.SemaphoreType.DMA((n_exp, f // blk))],
        compiler_params=pltpu.CompilerParams(vmem_limit_bytes=24_000_000),
        cost_estimate=pl.CostEstimate(flops=2 * n_exp * rows * d * f, bytes_accessed=4 * n_exp * d * f, transcendentals=0),
        name="grad_out",
    )(h, dz)


def combine_kernel(own, r1, l1, r2, l2, out):
    half = r2.shape[0]
    out[:half, :] = (own[:half, :] + l1[:half, :] + r2[...]).astype(BF16)
    out[half:, :] = (own[half:, :] + r1[half:, :] + l2[...]).astype(BF16)


def combine(own, r1, l1, r2, l2):
    return pl.pallas_call(
        combine_kernel,
        out_shape=jax.ShapeDtypeStruct(own.shape, BF16),
        in_specs=[pl.BlockSpec(memory_space=pltpu.VMEM)] * 5,
        out_specs=pl.BlockSpec(memory_space=pltpu.VMEM),
        compiler_params=pltpu.CompilerParams(vmem_limit_bytes=8_000_000),
        name="combine",
    )(own, r1, l1, r2, l2)


def solution(mesh):
    n_dev = mesh.shape["ep"]
    n_chip = n_dev // 2

    def local_step(x_loc, dy_loc, ids_loc, gate_loc, slot_loc, w_gate, w_down, w_up):
        tok, top_k = ids_loc.shape
        n_local = w_gate.shape[0]
        cap = slot_capacity(tok, top_k, n_local * n_dev)
        half = tok // 2
        xb, dz, h, da, db, r1, l1, ra, lb, own = run_exchange(
            x_loc, dy_loc, ids_loc.T, slot_loc.T, gate_loc.T, w_gate, w_up, w_down, n_dev, cap)
        to_right = [(c * 2 + k, (c + 1) % n_chip * 2 + k) for c in range(n_chip) for k in range(2)]
        to_left = [(b, a) for a, b in to_right]
        r1 = lax.ppermute(r1, "ep", to_right)
        l1 = lax.ppermute(l1, "ep", to_left)
        g_gate, g_up = grad_in(xb, da, db)
        g_gate, g_up, r1, l1 = lax.optimization_barrier((g_gate, g_up, r1, l1))
        r2 = lax.ppermute(ra + r1[:half], "ep", to_right)
        l2 = lax.ppermute(lb + l1[half:], "ep", to_left)
        g_down = grad_out(h, dz)
        dx = combine(own, r1, l1, r2, l2)
        return dx, g_gate, g_down, g_up

    tok_spec = P(("dp", "ep"), None)
    w_spec = P("ep", None, None)
    grad_spec = P(("dp", "ep"), None, None)
    return jax.shard_map(
        local_step, mesh=mesh,
        in_specs=(tok_spec,) * 5 + (w_spec,) * 3,
        out_specs=(tok_spec, grad_spec, grad_spec, grad_spec),
        check_vma=False)
```

```python
import functools

import jax
import jax.numpy as jnp
from jax import lax
from jax.experimental import pallas as pl
from jax.experimental.pallas import tpu as pltpu
from jax.sharding import PartitionSpec as P

F32 = jnp.float32
BF16 = jnp.bfloat16
NT = (((1,), (1,)), ((), ()))
TN = (((0,), (0,)), ((), ()))
DY_Q = 3
DX_COLS = (512, 512, 256, 256)
KEY_STRIDE = 256
N_COPIES = 45
OUT_TYPE = pltpu.VMEM


def slot_capacity(tok_dev, top_k, n_exp):
    return ((3 * tok_dev * top_k) // (2 * n_exp) + 7) // 8 * 8


def exchange_kernel(
    n_dev, cap,
    x_hbm, dy_hbm, ids_hbm, slot_hbm, gate_hbm, w1_hbm, w3_hbm, w2_hbm,
    xb, dz, hh, da, db, to_right, to_left, own,
    xg, dyg, ids, slots, gates_v, mt, w1, w3, w2, qq, uu, bb, dh, dxq,
    pm, pt, gm, part, sibr, far_out, far_in,
    loc_sem, w_sem, send, recv,
):
    n_exp = w1_hbm.shape[0]
    tok, d = x_hbm.shape
    half = tok // 2
    n_chip = n_dev // 2
    rc_rows = 2 * cap
    used = n_exp * rc_rows
    me = lax.axis_index("ep")
    chip, core = me // 2, lax.rem(me, 2)
    right = lax.rem(chip + 1, n_chip) * 2 + core
    left = lax.rem(chip + n_chip - 1, n_chip) * 2 + core
    sib = chip * 2 + 1 - core

    counter = [0]

    def remote(src, dst, dev):
        i = counter[0]
        counter[0] += 1
        return pltpu.make_async_remote_copy(
            src_ref=src, dst_ref=dst, send_sem=send.at[i], recv_sem=recv.at[i],
            device_id={"ep": dev}, device_id_type=pl.DeviceIdType.MESH)

    started = []

    def go(copy):
        copy.start()
        started.append(copy)
        return copy

    barrier = pltpu.get_barrier_semaphore()
    for dev in (right, left, sib):
        pl.semaphore_signal(barrier, inc=1, device_id={"ep": dev}, device_id_type=pl.DeviceIdType.MESH)

    loc = [
        pltpu.make_async_copy(src, dst, loc_sem.at[i])
        for i, (src, dst) in enumerate((
            (ids_hbm, ids), (slot_hbm, slots), (gate_hbm, gates_v),
            (x_hbm, xg.at[0, 0]), (dy_hbm, dyg.at[0, 0])))
    ]
    for c in loc:
        c.start()
    wcopies = {}
    for k, (src, dst) in enumerate(((w1_hbm, w1), (w3_hbm, w3))):
        for e in range(n_exp):
            wcopies[k, e] = pltpu.make_async_copy(src.at[e], dst.at[e], w_sem.at[k * n_exp + e])
    w2copy = pltpu.make_async_copy(w2_hbm, w2, w_sem.at[2 * n_exp])

    with jax.named_scope("head_keys"):
        for c in loc[:3]:
            c.wait()
        expert, slot = ids[...].astype(F32), slots[...].astype(F32)
        owner = jnp.floor((expert + 0.5) / float(n_exp))
        keys = owner * float(KEY_STRIDE) + (expert - owner * n_exp) * float(rc_rows) + slot
        keys = jnp.where(slot >= 0.0, keys, -1000.0)
        for i in range(2):
            mt[0, 0, :8, i * tok:(i + 1) * tok] = keys
            mt[0, 0, 8:, i * tok:(i + 1) * tok] = gates_v[...]

    with jax.named_scope("head_barrier"):
        pl.semaphore_wait(barrier, 3)

    rows_i = lax.broadcasted_iota(jnp.int32, (KEY_STRIDE, 2 * tok), 0)
    lane_i = lax.broadcasted_iota(jnp.int32, (16, 2 * tok), 1)
    row_key = (rows_i + me * KEY_STRIDE).astype(F32)

    def build(s):
        m0, m1 = mt[s, 0], mt[s, 1]
        first = lane_i < tok
        keys = jnp.where(first, m0, m1 + float(cap))
        gates = jnp.where(first, m0, m1)
        ones = jnp.zeros((KEY_STRIDE, 2 * tok), F32)
        gmat = jnp.zeros((KEY_STRIDE, 2 * tok), F32)
        for j in range(8):
            hit = row_key == keys[j:j + 1, :]
            ones = jnp.where(hit, 1.0, ones)
            gmat = jnp.where(hit, gates[8 + j:9 + j, :], gmat)
        pm[s] = ones.astype(BF16)
        pt[s] = jnp.transpose(ones).astype(BF16)
        gm[s] = jnp.sum(gmat, axis=1, keepdims=True)

    def gather_x(s):
        src = xg[s].reshape(2 * tok, d)
        rows = jnp.dot(pm[s, :used, :], src, preferred_element_type=F32).astype(BF16)
        for e in range(n_exp):
            xb[e, s * rc_rows:(s + 1) * rc_rows, :] = rows[e * rc_rows:(e + 1) * rc_rows, :]

    def gather_dy(s, c):
        src = dyg[s, :, :, c].reshape(2 * tok, c.stop - c.start)
        rows = jnp.dot(pm[s, :used, :], src, preferred_element_type=F32)
        rows = (rows * gm[s, :used, :]).astype(BF16)
        for e in range(n_exp):
            dz[e, s * rc_rows:(s + 1) * rc_rows, c] = rows[e * rc_rows:(e + 1) * rc_rows, :]

    def up(e):
        wcopies[0, e].wait()
        wcopies[1, e].wait()
        x = xb[e]
        a16 = jnp.dot(x, w1[e], preferred_element_type=F32).astype(BF16)
        b16 = jnp.dot(x, w3[e], preferred_element_type=F32).astype(BF16)
        a = a16.astype(F32)
        b = b16.astype(F32)
        sg = jax.nn.sigmoid(a)
        silu = a * sg
        hh[e] = (silu * b).astype(BF16)
        uu[e] = silu
        qq[e] = sg * (1.0 + a * (1.0 - sg))
        bb[e] = b16

    lo, hi = pl.ds(0, half), pl.ds(half, half)
    qd = d // DY_Q
    dcol = [slice(q * qd, (q + 1) * qd) for q in range(DY_Q)]
    full = slice(0, d)

    def far_cols(q):
        return pl.ds(q * qd, qd)

    m_r = go(remote(mt.at[0, 0], mt.at[3, 0], right))
    m_l = go(remote(mt.at[0, 0], mt.at[1, 0], left))
    m_s = go(remote(mt.at[0, 0], mt.at[0, 1], sib))
    loc[3].wait()
    xa_r = go(remote(xg.at[0, 0, lo], xg.at[3, 0, lo], right))
    xb_l = go(remote(xg.at[0, 0, hi], xg.at[1, 0, hi], left))
    xb_r = go(remote(xg.at[0, 0, hi], xg.at[3, 0, hi], right))
    xa_l = go(remote(xg.at[0, 0, lo], xg.at[1, 0, lo], left))
    x_s = go(remote(xg.at[0, 0], xg.at[0, 1], sib))
    loc[4].wait()
    y_s = go(remote(dyg.at[0, 0], dyg.at[0, 1], sib))
    for e in range(n_exp):
        wcopies[0, e].start()
        wcopies[1, e].start()
    w2copy.start()
    with jax.named_scope("own_rows"):
        m_s.wait_recv()
        build(0)
        m_r.wait_recv()
        m_rr = go(remote(mt.at[3, 0], mt.at[2, 0], right))
        m_s3 = go(remote(mt.at[3, 0], mt.at[3, 1], sib))
        m_l.wait_recv()
        m_s1 = go(remote(mt.at[1, 0], mt.at[1, 1], sib))
        x_s.wait_recv()
        gather_x(0)
    with jax.named_scope("x_relay"):
        xa_r.wait_recv()
        xa_rr = go(remote(xg.at[3, 0, lo], xg.at[2, 0, lo], right))
        xb_l.wait_recv()
        xb_ll = go(remote(xg.at[1, 0, hi], xg.at[2, 0, hi], left))
        ya_r = go(remote(dyg.at[0, 0, lo], dyg.at[3, 0, lo], right))
        yb_l = go(remote(dyg.at[0, 0, hi], dyg.at[1, 0, hi], left))
        yb_r = go(remote(dyg.at[0, 0, hi], dyg.at[3, 0, hi], right))
        ya_l = go(remote(dyg.at[0, 0, lo], dyg.at[1, 0, lo], left))
    with jax.named_scope("build31"):
        m_s3.wait_recv()
        build(3)
        m_s1.wait_recv()
        build(1)
    with jax.named_scope("x_near"):
        xb_r.wait_recv()
        x_s3 = go(remote(xg.at[3, 0], xg.at[3, 1], sib))
        xa_l.wait_recv()
        x_s1 = go(remote(xg.at[1, 0], xg.at[1, 1], sib))
        m_rr.wait_recv()
        m_s2 = go(remote(mt.at[2, 0], mt.at[2, 1], sib))
        y_s.wait_recv()
        gather_dy(0, full)
        x_s3.wait_recv()
        gather_x(3)
        x_s1.wait_recv()
        gather_x(1)
    with jax.named_scope("x_far"):
        m_s2.wait_recv()
        build(2)
        xa_rr.wait_recv()
        xb_ll.wait_recv()
        x_s2 = go(remote(xg.at[2, 0], xg.at[2, 1], sib))
        x_s2.wait_recv()
        gather_x(2)
    with jax.named_scope("up0"):
        up(0)
    with jax.named_scope("y_relay"):
        ya_r.wait_recv()
        yb_l.wait_recv()
        yfar = []
        for q in range(DY_Q):
            c = far_cols(q)
            yfar.append((go(remote(dyg.at[3, 0, lo, c], dyg.at[2, 0, lo, c], right)),
                         go(remote(dyg.at[1, 0, hi, c], dyg.at[2, 0, hi, c], left))))
    with jax.named_scope("up12"):
        up(1)
        up(2)
    with jax.named_scope("y_near_fwd"):
        yb_r.wait_recv()
        y_s3 = go(remote(dyg.at[3, 0], dyg.at[3, 1], sib))
        ya_l.wait_recv()
        y_s1 = go(remote(dyg.at[1, 0], dyg.at[1, 1], sib))
    with jax.named_scope("up34"):
        for e in range(3, n_exp):
            up(e)

    y_s2 = []

    def y_far_fwd(q):
        c = far_cols(q)
        for copy in yfar[q]:
            copy.wait_recv()
        y_s2.append(go(remote(dyg.at[2, 0, :, c], dyg.at[2, 1, :, c], sib)))

    with jax.named_scope("y_near"):
        y_far_fwd(0)
        y_s3.wait_recv()
        gather_dy(3, full)
        y_s1.wait_recv()
        gather_dy(1, full)

    def down(e, q):
        c = dcol[q]
        val = lax.dot_general(dz[e, :, c], w2[e, :, c], NT, preferred_element_type=F32)
        if q > 0:
            val = val + dh[e]
        if q < DY_Q - 1:
            dh[e] = val
        else:
            da[e] = (val * bb[e].astype(F32) * qq[e]).astype(BF16)
            db[e] = (val * uu[e]).astype(BF16)

    w2copy.wait()
    for q in range(DY_Q):
        with jax.named_scope(f"y_far{q}"):
            if q + 1 < DY_Q:
                y_far_fwd(q + 1)
            y_s2[q].wait_recv()
            gather_dy(2, dcol[q])
        with jax.named_scope(f"down{q}"):
            for e in range(n_exp):
                down(e, q)

    starts = [sum(DX_COLS[:q]) for q in range(len(DX_COLS))]
    sib_copies, far_copies = [], []

    def cols(q):
        return slice(starts[q], starts[q] + DX_COLS[q])

    def dx_block(q):
        c, w = cols(q), DX_COLS[q]
        for e in range(n_exp):
            v = lax.dot_general(da[e], w1[e, c, :], NT, preferred_element_type=F32)
            v = v + lax.dot_general(db[e], w3[e, c, :], NT, preferred_element_type=F32)
            dxq[e, :, :w] = v.astype(BF16)
        for s in range(n_chip):
            rows = dxq[:, s * rc_rows:(s + 1) * rc_rows, :w].reshape(used, w)
            part[s, :, :, c] = jnp.dot(pt[s, :, :used], rows, preferred_element_type=F32).reshape(2, tok, w)
        cs = pl.ds(starts[q], w)
        sib_copies.append(go(remote(part.at[:, 1, :, cs], sibr.at[:, :, cs], sib)))

    def total(s, rs, c):
        return part[s, 0, rs, c] + sibr[s, rs, c]

    a_rows, b_rows, all_rows = slice(0, half), slice(half, tok), slice(0, tok)

    def finish(q):
        c = cols(q)
        sib_copies[q].wait_recv()
        far_out[:, c] = total(2, all_rows, c)
        to_right[b_rows, c] = total(1, b_rows, c)
        to_left[a_rows, c] = total(3, a_rows, c)
        own[:, c] = total(0, all_rows, c)
        cs = pl.ds(starts[q], DX_COLS[q])
        far_copies.append((go(remote(far_out.at[lo, cs], far_in.at[lo, cs], right)),
                           go(remote(far_out.at[hi, cs], far_in.at[hi, cs], left))))

    def finish_far(q):
        c = cols(q)
        far_copies[q][0].wait_recv()
        to_right[a_rows, c] = total(1, a_rows, c) + far_in[a_rows, c]
        far_copies[q][1].wait_recv()
        to_left[b_rows, c] = total(3, b_rows, c) + far_in[b_rows, c]

    n_blocks = len(DX_COLS)
    for q in range(n_blocks):
        with jax.named_scope(f"dx{q}"):
            dx_block(q)
        if q >= 1:
            with jax.named_scope(f"finish{q - 1}"):
                finish(q - 1)
        if q >= 2:
            with jax.named_scope(f"far{q - 2}"):
                finish_far(q - 2)
    with jax.named_scope("finish_last"):
        finish(n_blocks - 1)
    with jax.named_scope("far_last"):
        finish_far(n_blocks - 2)
        finish_far(n_blocks - 1)
    with jax.named_scope("send_wait"):
        for c in started:
            c.wait_send()
    assert counter[0] == N_COPIES


def run_exchange(x, dy, ids, slots, gates, w1, w3, w2, n_dev, cap):
    n_exp, d, f = w1.shape
    tok = x.shape[0]
    n_chip = n_dev // 2
    rows = n_dev * cap
    any_spec = pl.BlockSpec(memory_space=pl.ANY)
    vmem_spec = pl.BlockSpec(memory_space=pltpu.VMEM)
    sds = OUT_TYPE
    outs = (
        sds((n_exp, rows, d), BF16), sds((n_exp, rows, d), BF16),
        sds((n_exp, rows, f), BF16), sds((n_exp, rows, f), BF16), sds((n_exp, rows, f), BF16),
        sds((tok, d), F32), sds((tok, d), F32), sds((tok, d), F32),
    )
    scratch = [
        pltpu.VMEM((n_chip, 2, tok, d), BF16),
        pltpu.VMEM((n_chip, 2, tok, d), BF16),
        pltpu.VMEM(ids.shape, jnp.int32),
        pltpu.VMEM(ids.shape, jnp.int32),
        pltpu.VMEM(ids.shape, F32),
        pltpu.VMEM((n_chip, 2, 16, 2 * tok), F32),
        pltpu.VMEM((n_exp, d, f), BF16),
        pltpu.VMEM((n_exp, d, f), BF16),
        pltpu.VMEM((n_exp, f, d), BF16),
        pltpu.VMEM((n_exp, rows, f), F32),
        pltpu.VMEM((n_exp, rows, f), F32),
        pltpu.VMEM((n_exp, rows, f), BF16),
        pltpu.VMEM((n_exp, rows, f), F32),
        pltpu.VMEM((n_exp, rows, max(DX_COLS)), BF16),
        pltpu.VMEM((n_chip, KEY_STRIDE, 2 * tok), BF16),
        pltpu.VMEM((n_chip, 2 * tok, KEY_STRIDE), BF16),
        pltpu.VMEM((n_chip, KEY_STRIDE, 1), F32),
        pltpu.VMEM((n_chip, 2, tok, d), F32),
        pltpu.VMEM((n_chip, tok, d), F32),
        pltpu.VMEM((tok, d), F32),
        pltpu.VMEM((tok, d), F32),
        pltpu.SemaphoreType.DMA((5,)),
        pltpu.SemaphoreType.DMA((2 * n_exp + 1,)),
        pltpu.SemaphoreType.DMA((N_COPIES,)),
        pltpu.SemaphoreType.DMA((N_COPIES,)),
    ]
    return pl.pallas_call(
        functools.partial(exchange_kernel, n_dev, cap),
        out_shape=outs,
        in_specs=[any_spec] * 8,
        out_specs=(vmem_spec,) * len(outs),
        scratch_shapes=scratch,
        compiler_params=pltpu.CompilerParams(
            collective_id=0, has_side_effects=True, vmem_limit_bytes=54_000_000),
        name="exchange",
    )(x, dy, ids, slots, gates, w1, w3, w2)


def grads_kernel(in_blk, out_blk, x, dz, h, da, db, g1_hbm, g3_hbm, g2_hbm, g1, g3, g2, sem):
    n_exp, rows, d = x.shape
    f = h.shape[2]
    pieces = [((g1, g1_hbm), k, in_blk) for k in range(d // in_blk)]
    pieces += [((g3, g3_hbm), k, in_blk) for k in range(d // in_blk)]
    pieces += [((g2, g2_hbm), k, out_blk) for k in range(f // out_blk)]

    n_in = d // in_blk
    depth = g2.shape[0]

    def store(e, i):
        (src, dst), k, blk = pieces[i]
        rs = pl.ds(k * blk, blk)
        slot = lax.rem(e, depth) if i >= 2 * n_in else e
        return pltpu.make_async_copy(src.at[slot, rs], dst.at[e, rs], sem.at[e, i])

    def step(e, carry):
        for k in range(n_in):
            rs = slice(k * in_blk, (k + 1) * in_blk)
            xt = x[e, :, rs]
            g1[e, rs, :] = lax.dot_general(xt, da[e], TN, preferred_element_type=F32)
            store(e, k).start()
            g3[e, rs, :] = lax.dot_general(xt, db[e], TN, preferred_element_type=F32)
            store(e, n_in + k).start()
        @pl.when(e >= depth)
        def _():
            for k in range(f // out_blk):
                store(e - depth, 2 * n_in + k).wait()

        for k in range(f // out_blk):
            rs = slice(k * out_blk, (k + 1) * out_blk)
            g2[lax.rem(e, depth), rs, :] = lax.dot_general(h[e, :, rs], dz[e], TN, preferred_element_type=F32)
            store(e, 2 * n_in + k).start()
        return carry

    lax.fori_loop(0, n_exp, step, 0)

    def drain(e, carry):
        for i in range(2 * n_in):
            store(e, i).wait()
        return carry

    lax.fori_loop(0, n_exp, drain, 0)
    for e in range(n_exp - depth, n_exp):
        for k in range(f // out_blk):
            store(e, 2 * n_in + k).wait()


def weight_grads(xb, dz, h, da, db, in_blk=512, out_blk=256):
    n_exp, rows, d = xb.shape
    f = da.shape[2]
    any_spec = pl.BlockSpec(memory_space=pl.ANY)
    g_in = jax.ShapeDtypeStruct((n_exp, d, f), F32)
    g_out = jax.ShapeDtypeStruct((n_exp, f, d), F32)
    n_pieces = 2 * (d // in_blk) + f // out_blk
    return pl.pallas_call(
        functools.partial(grads_kernel, in_blk, out_blk),
        out_shape=(g_in, g_in, g_out),
        in_specs=[pl.BlockSpec(memory_space=pltpu.VMEM)] * 5,
        out_specs=(any_spec,) * 3,
        scratch_shapes=[
            pltpu.VMEM(g_in.shape, F32), pltpu.VMEM(g_in.shape, F32), pltpu.VMEM((min(2, n_exp), f, d), F32),
            pltpu.SemaphoreType.DMA((n_exp, n_pieces))],
        compiler_params=pltpu.CompilerParams(vmem_limit_bytes=42_000_000),
        cost_estimate=pl.CostEstimate(flops=6 * n_exp * rows * d * f, bytes_accessed=12 * n_exp * d * f, transcendentals=0),
        name="weight_grads",
    )(xb, dz, h, da, db)


def combine_kernel(own, from_left, from_right, out):
    out[...] = (own[...] + from_left[...] + from_right[...]).astype(BF16)


def combine(own, from_left, from_right):
    return pl.pallas_call(
        combine_kernel,
        out_shape=jax.ShapeDtypeStruct(own.shape, BF16),
        in_specs=[pl.BlockSpec(memory_space=pltpu.VMEM)] * 3,
        out_specs=pl.BlockSpec(memory_space=pltpu.VMEM),
        compiler_params=pltpu.CompilerParams(vmem_limit_bytes=8_000_000),
        name="combine",
    )(own, from_left, from_right)


def solution(mesh):
    n_dev = mesh.shape["ep"]
    n_chip = n_dev // 2

    def local_step(x_loc, dy_loc, ids_loc, gate_loc, slot_loc, w_gate, w_down, w_up):
        tok, top_k = ids_loc.shape
        n_local = w_gate.shape[0]
        cap = slot_capacity(tok, top_k, n_local * n_dev)
        xb, dz, h, da, db, to_right, to_left, own = run_exchange(
            x_loc, dy_loc, ids_loc.T, slot_loc.T, gate_loc.T, w_gate, w_up, w_down, n_dev, cap)
        right_pairs = [(c * 2 + k, (c + 1) % n_chip * 2 + k) for c in range(n_chip) for k in range(2)]
        left_pairs = [(b, a) for a, b in right_pairs]
        from_left = lax.ppermute(to_right, "ep", right_pairs)
        from_right = lax.ppermute(to_left, "ep", left_pairs)
        g_gate, g_up, g_down = weight_grads(xb, dz, h, da, db)
        dx = combine(own, from_left, from_right)
        return dx, g_gate, g_down, g_up

    tok_spec = P(("dp", "ep"), None)
    w_spec = P("ep", None, None)
    grad_spec = P(("dp", "ep"), None, None)
    return jax.shard_map(
        local_step, mesh=mesh,
        in_specs=(tok_spec,) * 5 + (w_spec,) * 3,
        out_specs=(tok_spec, grad_spec, grad_spec, grad_spec),
        check_vma=False)
```

```python
import functools

import jax
import jax.numpy as jnp
from jax import lax
from jax.experimental import pallas as pl
from jax.experimental.pallas import tpu as pltpu
from jax.sharding import PartitionSpec as P

F32 = jnp.float32
BF16 = jnp.bfloat16
NT = (((1,), (1,)), ((), ()))
TN = (((0,), (0,)), ((), ()))
DY_Q = 3
DX_Q = 3
KEY_STRIDE = 256
N_COPIES = 57
N_GROUPS = 16
OUT_TYPE = pltpu.VMEM


def slot_capacity(tok_dev, top_k, n_exp):
    return ((3 * tok_dev * top_k) // (2 * n_exp) + 7) // 8 * 8


def exchange_kernel(
    n_dev, cap,
    x_hbm, dy_hbm, ids_hbm, slot_hbm, gate_hbm, w1_hbm, w3_hbm, w2_hbm,
    xb, dz, hh, da, db, r1, l1, ra, lb, own,
    xg, dyg, ids, slots, gates_v, mt, w1, w3, w2, qq, uu, bb, dh, dxq,
    pm, pt, gm, part, sibr,
    loc_sem, w_sem, send_sem, recv_sem,
):
    n_exp = w1_hbm.shape[0]
    tok, d = x_hbm.shape
    half = tok // 2
    n_chip = n_dev // 2
    rc_rows = 2 * cap
    used = n_exp * rc_rows
    me = lax.axis_index("ep")
    chip, core = me // 2, lax.rem(me, 2)
    right = lax.rem(chip + 1, n_chip) * 2 + core
    left = lax.rem(chip + n_chip - 1, n_chip) * 2 + core
    sib = chip * 2 + 1 - core

    counter = [0]

    groups = []

    def describe(src, dst, dev, send_i, recv_i):
        return pltpu.make_async_remote_copy(
            src_ref=src, dst_ref=dst, send_sem=send_sem.at[send_i], recv_sem=recv_sem.at[recv_i],
            device_id={"ep": dev}, device_id_type=pl.DeviceIdType.MESH)

    def go(src, dst, dev, group):
        if group not in groups:
            groups.append(group)
        copy = describe(src, dst, dev, groups.index(group), counter[0])
        counter[0] += 1
        copy.start()
        return copy

    barrier = pltpu.get_barrier_semaphore()
    for dev in (right, left, sib):
        pl.semaphore_signal(barrier, inc=1, device_id={"ep": dev}, device_id_type=pl.DeviceIdType.MESH)

    loc = [
        pltpu.make_async_copy(src, dst, loc_sem.at[i])
        for i, (src, dst) in enumerate((
            (ids_hbm, ids), (slot_hbm, slots), (gate_hbm, gates_v),
            (x_hbm, xg.at[0, 0]), (dy_hbm, dyg.at[0, 0])))
    ]
    for c in loc:
        c.start()
    wcopies = {}
    for k, (src, dst) in enumerate(((w1_hbm, w1), (w3_hbm, w3))):
        for e in range(n_exp):
            wcopies[k, e] = pltpu.make_async_copy(src.at[e], dst.at[e], w_sem.at[k * n_exp + e])
    w2copy = pltpu.make_async_copy(w2_hbm, w2, w_sem.at[2 * n_exp])

    with jax.named_scope("head_keys"):
        for c in loc[:3]:
            c.wait()
        expert, slot = ids[...].astype(F32), slots[...].astype(F32)
        owner = jnp.floor((expert + 0.5) / float(n_exp))
        keys = owner * float(KEY_STRIDE) + (expert - owner * n_exp) * float(rc_rows) + slot
        keys = jnp.where(slot >= 0.0, keys, -1000.0)
        for i in range(2):
            mt[0, 0, :8, i * tok:(i + 1) * tok] = keys
            mt[0, 0, 8:, i * tok:(i + 1) * tok] = gates_v[...]

    with jax.named_scope("head_barrier"):
        pl.semaphore_wait(barrier, 3)

    rows_i = lax.broadcasted_iota(jnp.int32, (KEY_STRIDE, 2 * tok), 0)
    lane_i = lax.broadcasted_iota(jnp.int32, (16, 2 * tok), 1)
    row_key = (rows_i + me * KEY_STRIDE).astype(F32)

    def build(s):
        m0, m1 = mt[s, 0], mt[s, 1]
        first = lane_i < tok
        keys = jnp.where(first, m0, m1 + float(cap))
        gates = jnp.where(first, m0, m1)
        ones = jnp.zeros((KEY_STRIDE, 2 * tok), F32)
        gmat = jnp.zeros((KEY_STRIDE, 2 * tok), F32)
        for j in range(8):
            hit = row_key == keys[j:j + 1, :]
            ones = jnp.where(hit, 1.0, ones)
            gmat = jnp.where(hit, gates[8 + j:9 + j, :], gmat)
        pm[s] = ones.astype(BF16)
        pt[s] = jnp.transpose(ones).astype(BF16)
        gm[s] = jnp.sum(gmat, axis=1, keepdims=True)

    def gather_x(s, c):
        src = xg[s, :, :, c].reshape(2 * tok, c.stop - c.start)
        rows = jnp.dot(pm[s, :used, :], src, preferred_element_type=F32).astype(BF16)
        for e in range(n_exp):
            xb[e, s * rc_rows:(s + 1) * rc_rows, c] = rows[e * rc_rows:(e + 1) * rc_rows, :]

    def gather_dy(s, c):
        src = dyg[s, :, :, c].reshape(2 * tok, c.stop - c.start)
        rows = jnp.dot(pm[s, :used, :], src, preferred_element_type=F32)
        rows = (rows * gm[s, :used, :]).astype(BF16)
        for e in range(n_exp):
            dz[e, s * rc_rows:(s + 1) * rc_rows, c] = rows[e * rc_rows:(e + 1) * rc_rows, :]

    hcol = [slice(0, d // 2), slice(d // 2, d)]

    def up_first(e):
        wcopies[0, e].wait()
        wcopies[1, e].wait()
        x = xb[e, :, hcol[0]]
        qq[e] = jnp.dot(x, w1[e, hcol[0], :], preferred_element_type=F32)
        uu[e] = jnp.dot(x, w3[e, hcol[0], :], preferred_element_type=F32)

    def up_second(e):
        x = xb[e, :, hcol[1]]
        a16 = (qq[e] + jnp.dot(x, w1[e, hcol[1], :], preferred_element_type=F32)).astype(BF16)
        b16 = (uu[e] + jnp.dot(x, w3[e, hcol[1], :], preferred_element_type=F32)).astype(BF16)
        a = a16.astype(F32)
        b = b16.astype(F32)
        sg = jax.nn.sigmoid(a)
        silu = a * sg
        hh[e] = (silu * b).astype(BF16)
        uu[e] = silu
        qq[e] = sg * (1.0 + a * (1.0 - sg))
        bb[e] = b16

    lo, hi = pl.ds(0, half), pl.ds(half, half)
    qd = d // DY_Q
    dcol = [slice(q * qd, (q + 1) * qd) for q in range(DY_Q)]
    full = slice(0, d)

    def label(buf, kind):
        return ("x" if buf is xg else "y") + kind

    def send(buf, slot, rows, c, dev_slot, dev, kind):
        cs = pl.ds(c.start, c.stop - c.start)
        return go(buf.at[slot, 0, rows, cs], buf.at[dev_slot, 0, rows, cs], dev, label(buf, kind))

    def forward(buf, slot, c):
        cs = pl.ds(c.start, c.stop - c.start)
        return go(buf.at[slot, 0, :, cs], buf.at[slot, 1, :, cs], sib, label(buf, "s"))

    def to_right(buf, rows, c):
        return send(buf, 0, rows, c, 3, right, "r")

    def to_left(buf, rows, c):
        return send(buf, 0, rows, c, 1, left, "l")

    x, y = {}, {}

    def near_pair(t, buf, c, k, first):
        if first:
            t["ar", k], t["bl", k] = to_right(buf, lo, c), to_left(buf, hi, c)
        else:
            t["br", k], t["al", k] = to_right(buf, hi, c), to_left(buf, lo, c)

    def relay(t, buf, c, k):
        t["ar", k].wait_recv()
        t["arr", k] = send(buf, 3, lo, c, 2, right, "rr")
        t["bl", k].wait_recv()
        t["bll", k] = send(buf, 1, hi, c, 2, left, "ll")

    def near_forward(t, buf, c, k):
        t["br", k].wait_recv()
        t["s3", k] = forward(buf, 3, c)
        t["al", k].wait_recv()
        t["s1", k] = forward(buf, 1, c)

    def far_forward(t, buf, c, k):
        t["arr", k].wait_recv()
        t["bll", k].wait_recv()
        t["s2", k] = forward(buf, 2, c)

    m_r = go(mt.at[0, 0], mt.at[3, 0], right, "mr")
    m_l = go(mt.at[0, 0], mt.at[1, 0], left, "ml")
    m_s = go(mt.at[0, 0], mt.at[0, 1], sib, "ms")
    loc[3].wait()
    near_pair(x, xg, hcol[0], 0, True)
    near_pair(x, xg, hcol[0], 0, False)
    near_pair(x, xg, hcol[1], 1, True)
    x["s0", 0] = forward(xg, 0, full)
    loc[4].wait()
    y["s0", 0] = forward(dyg, 0, full)
    for e in range(n_exp):
        wcopies[0, e].start()
        wcopies[1, e].start()
    w2copy.start()
    with jax.named_scope("own_rows"):
        m_s.wait_recv()
        build(0)
        m_r.wait_recv()
        m_rr = go(mt.at[3, 0], mt.at[2, 0], right, "mr")
        m_s3 = go(mt.at[3, 0], mt.at[3, 1], sib, "ms")
        m_l.wait_recv()
        m_s1 = go(mt.at[1, 0], mt.at[1, 1], sib, "ms")
        x["s0", 0].wait_recv()
        gather_x(0, full)
    with jax.named_scope("x_relay0"):
        relay(x, xg, hcol[0], 0)
        near_pair(x, xg, hcol[1], 1, False)
    with jax.named_scope("build3"):
        m_s3.wait_recv()
        build(3)
    with jax.named_scope("x_near_fwd0"):
        near_forward(x, xg, hcol[0], 0)
    with jax.named_scope("x_relay1"):
        relay(x, xg, hcol[1], 1)
        for k in (0, 1):
            near_pair(y, dyg, dcol[k], k, True)
            near_pair(y, dyg, dcol[k], k, False)
        m_rr.wait_recv()
        m_s2 = go(mt.at[2, 0], mt.at[2, 1], sib, "ms")
    with jax.named_scope("build1"):
        m_s1.wait_recv()
        build(1)
        x["s3", 0].wait_recv()
        gather_x(3, hcol[0])
        x["s1", 0].wait_recv()
        gather_x(1, hcol[0])
    with jax.named_scope("x_far_fwd0"):
        far_forward(x, xg, hcol[0], 0)
    with jax.named_scope("build2"):
        m_s2.wait_recv()
        build(2)
    with jax.named_scope("x_near_fwd1"):
        near_forward(x, xg, hcol[1], 1)
    with jax.named_scope("x_far0"):
        x["s2", 0].wait_recv()
        gather_x(2, hcol[0])
    with jax.named_scope("up_first01"):
        up_first(0)
        up_first(1)
    with jax.named_scope("x_far_fwd1"):
        far_forward(x, xg, hcol[1], 1)
    with jax.named_scope("up_first234"):
        for e in range(2, n_exp):
            up_first(e)
    with jax.named_scope("y_relay0"):
        relay(y, dyg, dcol[0], 0)
        near_pair(y, dyg, dcol[2], 2, True)
        near_pair(y, dyg, dcol[2], 2, False)
        near_forward(y, dyg, dcol[0], 0)
    with jax.named_scope("x_rest"):
        for slot in (3, 1, 2):
            x["s%d" % slot, 1].wait_recv()
            gather_x(slot, hcol[1])
    with jax.named_scope("up_second01"):
        up_second(0)
        up_second(1)
    with jax.named_scope("y_relay1"):
        relay(y, dyg, dcol[1], 1)
        near_forward(y, dyg, dcol[1], 1)
    with jax.named_scope("up_second23"):
        up_second(2)
        up_second(3)
    with jax.named_scope("y_far_fwd0"):
        far_forward(y, dyg, dcol[0], 0)
    with jax.named_scope("up_second4"):
        for e in range(4, n_exp):
            up_second(e)
    with jax.named_scope("y_relay2"):
        relay(y, dyg, dcol[2], 2)
        y["s0", 0].wait_recv()
        gather_dy(0, full)

    def down(e, q):
        c = dcol[q]
        val = lax.dot_general(dz[e, :, c], w2[e, :, c], NT, preferred_element_type=F32)
        if q > 0:
            val = val + dh[e]
        if q < DY_Q - 1:
            dh[e] = val
        else:
            da[e] = (val * bb[e].astype(F32) * qq[e]).astype(BF16)
            db[e] = (val * uu[e]).astype(BF16)

    w2copy.wait()
    for q in range(DY_Q):
        with jax.named_scope(f"y_near{q}"):
            for slot in (3, 1):
                y["s%d" % slot, q].wait_recv()
                gather_dy(slot, dcol[q])
        with jax.named_scope(f"y_fwd{q}"):
            if q == 0:
                near_forward(y, dyg, dcol[2], 2)
            if q == 1:
                far_forward(y, dyg, dcol[2], 2)
        with jax.named_scope(f"y_far{q}"):
            y["s2", q].wait_recv()
            gather_dy(2, dcol[q])
        with jax.named_scope(f"down{q}"):
            for e in range(n_exp):
                down(e, q)
        if q == 0:
            with jax.named_scope("y_far_fwd1"):
                far_forward(y, dyg, dcol[1], 1)

    qx = d // DX_Q
    sib_copies = []

    def dx_block(q):
        c = slice(q * qx, (q + 1) * qx)
        for e in range(n_exp):
            v = lax.dot_general(da[e], w1[e, c, :], NT, preferred_element_type=F32)
            v = v + lax.dot_general(db[e], w3[e, c, :], NT, preferred_element_type=F32)
            dxq[e] = v.astype(BF16)
        for s in range(n_chip):
            rows = dxq[:, s * rc_rows:(s + 1) * rc_rows, :].reshape(used, qx)
            part[q, s] = jnp.dot(pt[s, :, :used], rows, preferred_element_type=F32).reshape(2, tok, qx)
        sib_copies.append(go(part.at[q, :, 1], sibr.at[q], sib, "p%d" % q))

    def finish(q):
        c = slice(q * qx, (q + 1) * qx)
        sib_copies[q].wait_recv()

        def total(s, rs):
            return part[q, s, 0, rs] + sibr[q, s, rs]

        a, b = slice(0, half), slice(half, tok)
        r1[a, c] = total(2, a)
        r1[b, c] = total(1, b)
        l1[a, c] = total(3, a)
        l1[b, c] = total(2, b)
        ra[:, c] = total(1, a)
        lb[:, c] = total(3, b)
        own[:, c] = part[q, 0, 0] + sibr[q, 0]

    for q in range(DX_Q):
        with jax.named_scope(f"dx{q}"):
            dx_block(q)
        if q > 0:
            with jax.named_scope(f"finish{q - 1}"):
                finish(q - 1)
    with jax.named_scope(f"finish{DX_Q - 1}"):
        finish(DX_Q - 1)

    with jax.named_scope("send_wait"):
        whole = {"mr": mt.at[0], "ml": mt.at[0, 0], "ms": mt.at[:, 0]}
        for name, buf in (("x", xg), ("y", dyg)):
            whole.update({name + "r": buf.at[0, 0], name + "l": buf.at[0, 0], name + "s": buf.at[:, 0],
                          name + "rr": buf.at[0, 0, lo], name + "ll": buf.at[0, 0, hi]})
        for q in range(DX_Q):
            whole["p%d" % q] = part.at[q, :, 1]
        for i, group in enumerate(groups):
            describe(whole[group], whole[group], sib, i, 0).wait_send()
    assert (counter[0], len(groups)) == (N_COPIES, N_GROUPS)


def run_exchange(x, dy, ids, slots, gates, w1, w3, w2, n_dev, cap):
    n_exp, d, f = w1.shape
    tok = x.shape[0]
    half = tok // 2
    n_chip = n_dev // 2
    rows = n_dev * cap
    used = n_exp * 2 * cap
    qx = d // DX_Q
    any_spec = pl.BlockSpec(memory_space=pl.ANY)
    vmem_spec = pl.BlockSpec(memory_space=pltpu.VMEM)
    sds = OUT_TYPE
    outs = (
        sds((n_exp, rows, d), BF16), sds((n_exp, rows, d), BF16),
        sds((n_exp, rows, f), BF16), sds((n_exp, rows, f), BF16), sds((n_exp, rows, f), BF16),
        sds((tok, d), F32), sds((tok, d), F32), sds((half, d), F32), sds((half, d), F32), sds((tok, d), F32),
    )
    scratch = [
        pltpu.VMEM((n_chip, 2, tok, d), BF16),
        pltpu.VMEM((n_chip, 2, tok, d), BF16),
        pltpu.VMEM(ids.shape, jnp.int32),
        pltpu.VMEM(ids.shape, jnp.int32),
        pltpu.VMEM(ids.shape, F32),
        pltpu.VMEM((n_chip, 2, 16, 2 * tok), F32),
        pltpu.VMEM((n_exp, d, f), BF16),
        pltpu.VMEM((n_exp, d, f), BF16),
        pltpu.VMEM((n_exp, f, d), BF16),
        pltpu.VMEM((n_exp, rows, f), F32),
        pltpu.VMEM((n_exp, rows, f), F32),
        pltpu.VMEM((n_exp, rows, f), BF16),
        pltpu.VMEM((n_exp, rows, f), F32),
        pltpu.VMEM((n_exp, rows, qx), BF16),
        pltpu.VMEM((n_chip, KEY_STRIDE, 2 * tok), BF16),
        pltpu.VMEM((n_chip, 2 * tok, KEY_STRIDE), BF16),
        pltpu.VMEM((n_chip, KEY_STRIDE, 1), F32),
        pltpu.VMEM((DX_Q, n_chip, 2, tok, qx), F32),
        pltpu.VMEM((DX_Q, n_chip, tok, qx), F32),
        pltpu.SemaphoreType.DMA((5,)),
        pltpu.SemaphoreType.DMA((2 * n_exp + 1,)),
        pltpu.SemaphoreType.DMA((N_GROUPS,)),
        pltpu.SemaphoreType.DMA((N_COPIES,)),
    ]
    return pl.pallas_call(
        functools.partial(exchange_kernel, n_dev, cap),
        out_shape=outs,
        in_specs=[any_spec] * 8,
        out_specs=(vmem_spec,) * len(outs),
        scratch_shapes=scratch,
        compiler_params=pltpu.CompilerParams(
            collective_id=0, has_side_effects=True, vmem_limit_bytes=54_000_000),
        name="exchange",
    )(x, dy, ids, slots, gates, w1, w3, w2)


def grad_in_kernel(blk, x, da, db, g1_hbm, g3_hbm, g1, g3, sem):
    n_exp, rows, d = x.shape
    n_blk = d // blk

    def store(e, k):
        rs = pl.ds(k * blk, blk)
        return [pltpu.make_async_copy(src.at[e, rs], dst.at[e, rs], sem.at[o, e, k])
                for o, (src, dst) in enumerate(((g1, g1_hbm), (g3, g3_hbm)))]

    def step(e, carry):
        for k in range(n_blk):
            rs = slice(k * blk, (k + 1) * blk)
            xt = x[e, :, rs]
            g1[e, rs, :] = lax.dot_general(xt, da[e], TN, preferred_element_type=F32)
            g3[e, rs, :] = lax.dot_general(xt, db[e], TN, preferred_element_type=F32)
            for c in store(e, k):
                c.start()
        return carry

    lax.fori_loop(0, n_exp, step, 0)

    def drain(e, carry):
        for k in range(n_blk):
            for c in store(e, k):
                c.wait()
        return carry

    lax.fori_loop(0, n_exp, drain, 0)


def grad_in(xb, da, db, blk=512):
    n_exp, rows, d = xb.shape
    f = da.shape[2]
    any_spec = pl.BlockSpec(memory_space=pl.ANY)
    out = jax.ShapeDtypeStruct((n_exp, d, f), F32)
    return pl.pallas_call(
        functools.partial(grad_in_kernel, blk),
        out_shape=(out, out),
        in_specs=[pl.BlockSpec(memory_space=pltpu.VMEM)] * 3,
        out_specs=(any_spec, any_spec),
        scratch_shapes=[
            pltpu.VMEM(out.shape, F32), pltpu.VMEM(out.shape, F32),
            pltpu.SemaphoreType.DMA((2, n_exp, d // blk))],
        compiler_params=pltpu.CompilerParams(vmem_limit_bytes=40_000_000),
        cost_estimate=pl.CostEstimate(flops=4 * n_exp * rows * d * f, bytes_accessed=8 * n_exp * d * f, transcendentals=0),
        name="grad_in",
    )(xb, da, db)


def grad_out_kernel(blk, h, dz, g_hbm, g, sem):
    n_exp, rows, f = h.shape
    n_blk = f // blk

    def store(e, k):
        rs = pl.ds(k * blk, blk)
        return pltpu.make_async_copy(g.at[e, rs], g_hbm.at[e, rs], sem.at[e, k])

    def step(e, carry):
        for k in range(n_blk):
            rs = slice(k * blk, (k + 1) * blk)
            g[e, rs, :] = lax.dot_general(h[e, :, rs], dz[e], TN, preferred_element_type=F32)
            store(e, k).start()
        return carry

    lax.fori_loop(0, n_exp, step, 0)

    def drain(e, carry):
        for k in range(n_blk):
            store(e, k).wait()
        return carry

    lax.fori_loop(0, n_exp, drain, 0)


def grad_out(h, dz, blk=256):
    n_exp, rows, f = h.shape
    d = dz.shape[2]
    out = jax.ShapeDtypeStruct((n_exp, f, d), F32)
    return pl.pallas_call(
        functools.partial(grad_out_kernel, blk),
        out_shape=out,
        in_specs=[pl.BlockSpec(memory_space=pltpu.VMEM)] * 2,
        out_specs=pl.BlockSpec(memory_space=pl.ANY),
        scratch_shapes=[pltpu.VMEM(out.shape, F32), pltpu.SemaphoreType.DMA((n_exp, f // blk))],
        compiler_params=pltpu.CompilerParams(vmem_limit_bytes=24_000_000),
        cost_estimate=pl.CostEstimate(flops=2 * n_exp * rows * d * f, bytes_accessed=4 * n_exp * d * f, transcendentals=0),
        name="grad_out",
    )(h, dz)


def combine_kernel(own, r1, l1, r2, l2, out):
    half = r2.shape[0]
    out[:half, :] = (own[:half, :] + l1[:half, :] + r2[...]).astype(BF16)
    out[half:, :] = (own[half:, :] + r1[half:, :] + l2[...]).astype(BF16)


def combine(own, r1, l1, r2, l2):
    return pl.pallas_call(
        combine_kernel,
        out_shape=jax.ShapeDtypeStruct(own.shape, BF16),
        in_specs=[pl.BlockSpec(memory_space=pltpu.VMEM)] * 5,
        out_specs=pl.BlockSpec(memory_space=pltpu.VMEM),
        compiler_params=pltpu.CompilerParams(vmem_limit_bytes=8_000_000),
        name="combine",
    )(own, r1, l1, r2, l2)


def solution(mesh):
    n_dev = mesh.shape["ep"]
    n_chip = n_dev // 2

    def local_step(x_loc, dy_loc, ids_loc, gate_loc, slot_loc, w_gate, w_down, w_up):
        tok, top_k = ids_loc.shape
        n_local = w_gate.shape[0]
        cap = slot_capacity(tok, top_k, n_local * n_dev)
        half = tok // 2
        xb, dz, h, da, db, r1, l1, ra, lb, own = run_exchange(
            x_loc, dy_loc, ids_loc.T, slot_loc.T, gate_loc.T, w_gate, w_up, w_down, n_dev, cap)
        to_right = [(c * 2 + k, (c + 1) % n_chip * 2 + k) for c in range(n_chip) for k in range(2)]
        to_left = [(b, a) for a, b in to_right]
        r1 = lax.ppermute(r1, "ep", to_right)
        l1 = lax.ppermute(l1, "ep", to_left)
        g_gate, g_up = grad_in(xb, da, db)
        g_gate, g_up, r1, l1 = lax.optimization_barrier((g_gate, g_up, r1, l1))
        r2 = lax.ppermute(ra + r1[:half], "ep", to_right)
        l2 = lax.ppermute(lb + l1[half:], "ep", to_left)
        g_down = grad_out(h, dz)
        dx = combine(own, r1, l1, r2, l2)
        return dx, g_gate, g_down, g_up

    tok_spec = P(("dp", "ep"), None)
    w_spec = P("ep", None, None)
    grad_spec = P(("dp", "ep"), None, None)
    return jax.shard_map(
        local_step, mesh=mesh,
        in_specs=(tok_spec,) * 5 + (w_spec,) * 3,
        out_specs=(tok_spec, grad_spec, grad_spec, grad_spec),
        check_vma=False)
```

```python
import functools

import jax
import jax.numpy as jnp
from jax import lax
from jax.experimental import pallas as pl
from jax.experimental.pallas import tpu as pltpu
from jax.sharding import PartitionSpec as P

F32 = jnp.float32
BF16 = jnp.bfloat16
NT = (((1,), (1,)), ((), ()))
TN = (((0,), (0,)), ((), ()))
DY_Q = 3
DX_Q = 3
KEY_STRIDE = 256
N_COPIES = 36
N_GROUPS = 16
OUT_TYPE = pltpu.VMEM


def slot_capacity(tok_dev, top_k, n_exp):
    return ((3 * tok_dev * top_k) // (2 * n_exp) + 7) // 8 * 8


def exchange_kernel(
    n_dev, cap,
    x_hbm, dy_hbm, ids_hbm, slot_hbm, gate_hbm, w1_hbm, w3_hbm, w2_hbm,
    xb, dz, hh, da, db, r1, l1, ra, lb, own,
    xg, dyg, ids, slots, gates_v, mt, w1, w3, w2, qq, uu, bb, dh, dxq,
    pm, pt, gm, part, sibr,
    loc_sem, w_sem, send_sem, recv_sem,
):
    n_exp = w1_hbm.shape[0]
    tok, d = x_hbm.shape
    half = tok // 2
    n_chip = n_dev // 2
    rc_rows = 2 * cap
    used = n_exp * rc_rows
    me = lax.axis_index("ep")
    chip, core = me // 2, lax.rem(me, 2)
    right = lax.rem(chip + 1, n_chip) * 2 + core
    left = lax.rem(chip + n_chip - 1, n_chip) * 2 + core
    sib = chip * 2 + 1 - core

    counter = [0]

    groups = []

    def describe(src, dst, dev, send_i, recv_i):
        return pltpu.make_async_remote_copy(
            src_ref=src, dst_ref=dst, send_sem=send_sem.at[send_i], recv_sem=recv_sem.at[recv_i],
            device_id={"ep": dev}, device_id_type=pl.DeviceIdType.MESH)

    def go(src, dst, dev, group):
        if group not in groups:
            groups.append(group)
        copy = describe(src, dst, dev, groups.index(group), counter[0])
        counter[0] += 1
        copy.start()
        return copy

    barrier = pltpu.get_barrier_semaphore()
    for dev in (right, left, sib):
        pl.semaphore_signal(barrier, inc=1, device_id={"ep": dev}, device_id_type=pl.DeviceIdType.MESH)

    loc = [
        pltpu.make_async_copy(src, dst, loc_sem.at[i])
        for i, (src, dst) in enumerate((
            (ids_hbm, ids), (slot_hbm, slots), (gate_hbm, gates_v),
            (x_hbm, xg.at[0, 0]), (dy_hbm, dyg.at[0, 0])))
    ]
    for c in loc:
        c.start()
    wcopies = {}
    for k, (src, dst) in enumerate(((w1_hbm, w1), (w3_hbm, w3))):
        for e in range(n_exp):
            wcopies[k, e] = pltpu.make_async_copy(src.at[e], dst.at[e], w_sem.at[k * n_exp + e])
    w2copy = pltpu.make_async_copy(w2_hbm, w2, w_sem.at[2 * n_exp])

    with jax.named_scope("head_keys"):
        for c in loc[:3]:
            c.wait()
        expert, slot = ids[...].astype(F32), slots[...].astype(F32)
        owner = jnp.floor((expert + 0.5) / float(n_exp))
        keys = owner * float(KEY_STRIDE) + (expert - owner * n_exp) * float(rc_rows) + slot
        keys = jnp.where(slot >= 0.0, keys, -1000.0)
        for i in range(2):
            mt[0, 0, :8, i * tok:(i + 1) * tok] = keys
            mt[0, 0, 8:, i * tok:(i + 1) * tok] = gates_v[...]

    with jax.named_scope("head_barrier"):
        pl.semaphore_wait(barrier, 3)

    rows_i = lax.broadcasted_iota(jnp.int32, (KEY_STRIDE, 2 * tok), 0)
    lane_i = lax.broadcasted_iota(jnp.int32, (16, 2 * tok), 1)
    row_key = (rows_i + me * KEY_STRIDE).astype(F32)

    def build(s):
        m0, m1 = mt[s, 0], mt[s, 1]
        first = lane_i < tok
        keys = jnp.where(first, m0, m1 + float(cap))
        gates = jnp.where(first, m0, m1)
        ones = jnp.zeros((KEY_STRIDE, 2 * tok), F32)
        gmat = jnp.zeros((KEY_STRIDE, 2 * tok), F32)
        for j in range(8):
            hit = row_key == keys[j:j + 1, :]
            ones = jnp.where(hit, 1.0, ones)
            gmat = jnp.where(hit, gates[8 + j:9 + j, :], gmat)
        pm[s] = ones.astype(BF16)
        pt[s] = jnp.transpose(ones).astype(BF16)
        gm[s] = jnp.sum(gmat, axis=1, keepdims=True)

    def gather_x(s):
        src = xg[s].reshape(2 * tok, d)
        rows = jnp.dot(pm[s, :used, :], src, preferred_element_type=F32).astype(BF16)
        for e in range(n_exp):
            xb[e, s * rc_rows:(s + 1) * rc_rows, :] = rows[e * rc_rows:(e + 1) * rc_rows, :]

    def gather_dy(s, c):
        src = dyg[s, :, :, c].reshape(2 * tok, c.stop - c.start)
        rows = jnp.dot(pm[s, :used, :], src, preferred_element_type=F32)
        rows = (rows * gm[s, :used, :]).astype(BF16)
        for e in range(n_exp):
            dz[e, s * rc_rows:(s + 1) * rc_rows, c] = rows[e * rc_rows:(e + 1) * rc_rows, :]

    def up(e):
        wcopies[0, e].wait()
        wcopies[1, e].wait()
        x = xb[e]
        a16 = jnp.dot(x, w1[e], preferred_element_type=F32).astype(BF16)
        b16 = jnp.dot(x, w3[e], preferred_element_type=F32).astype(BF16)
        a = a16.astype(F32)
        b = b16.astype(F32)
        sg = jax.nn.sigmoid(a)
        silu = a * sg
        hh[e] = (silu * b).astype(BF16)
        uu[e] = silu
        qq[e] = sg * (1.0 + a * (1.0 - sg))
        bb[e] = b16

    lo, hi = pl.ds(0, half), pl.ds(half, half)
    qd = d // DY_Q
    dcol = [slice(q * qd, (q + 1) * qd) for q in range(DY_Q)]
    full = slice(0, d)

    def far_cols(q):
        return pl.ds(q * qd, qd)

    m_r = go(mt.at[0, 0], mt.at[3, 0], right, "mr")
    m_l = go(mt.at[0, 0], mt.at[1, 0], left, "ml")
    m_s = go(mt.at[0, 0], mt.at[0, 1], sib, "ms")
    loc[3].wait()
    xa_r = go(xg.at[0, 0, lo], xg.at[3, 0, lo], right, "xr")
    xb_l = go(xg.at[0, 0, hi], xg.at[1, 0, hi], left, "xl")
    xb_r = go(xg.at[0, 0, hi], xg.at[3, 0, hi], right, "xr")
    xa_l = go(xg.at[0, 0, lo], xg.at[1, 0, lo], left, "xl")
    x_s = go(xg.at[0, 0], xg.at[0, 1], sib, "xs")
    loc[4].wait()
    y_s = go(dyg.at[0, 0], dyg.at[0, 1], sib, "ys")
    for e in range(n_exp):
        wcopies[0, e].start()
        wcopies[1, e].start()
    w2copy.start()
    with jax.named_scope("own_rows"):
        m_s.wait_recv()
        build(0)
        m_r.wait_recv()
        m_rr = go(mt.at[3, 0], mt.at[2, 0], right, "mr")
        m_s3 = go(mt.at[3, 0], mt.at[3, 1], sib, "ms")
        m_l.wait_recv()
        m_s1 = go(mt.at[1, 0], mt.at[1, 1], sib, "ms")
        x_s.wait_recv()
        gather_x(0)
    with jax.named_scope("x_relay"):
        xa_r.wait_recv()
        xa_rr = go(xg.at[3, 0, lo], xg.at[2, 0, lo], right, "xrr")
        xb_l.wait_recv()
        xb_ll = go(xg.at[1, 0, hi], xg.at[2, 0, hi], left, "xll")
        ya_r = go(dyg.at[0, 0, lo], dyg.at[3, 0, lo], right, "yr")
        yb_l = go(dyg.at[0, 0, hi], dyg.at[1, 0, hi], left, "yl")
        yb_r = go(dyg.at[0, 0, hi], dyg.at[3, 0, hi], right, "yr")
        ya_l = go(dyg.at[0, 0, lo], dyg.at[1, 0, lo], left, "yl")
    with jax.named_scope("build31"):
        m_s3.wait_recv()
        build(3)
        m_s1.wait_recv()
        build(1)
    with jax.named_scope("x_near"):
        xb_r.wait_recv()
        x_s3 = go(xg.at[3, 0], xg.at[3, 1], sib, "xs")
        xa_l.wait_recv()
        x_s1 = go(xg.at[1, 0], xg.at[1, 1], sib, "xs")
        m_rr.wait_recv()
        m_s2 = go(mt.at[2, 0], mt.at[2, 1], sib, "ms")
        y_s.wait_recv()
        gather_dy(0, full)
        x_s3.wait_recv()
        gather_x(3)
        x_s1.wait_recv()
        gather_x(1)
    with jax.named_scope("x_far"):
        m_s2.wait_recv()
        build(2)
        xa_rr.wait_recv()
        xb_ll.wait_recv()
        x_s2 = go(xg.at[2, 0], xg.at[2, 1], sib, "xs")
        x_s2.wait_recv()
        gather_x(2)
    with jax.named_scope("up0"):
        up(0)
    with jax.named_scope("y_relay"):
        ya_r.wait_recv()
        yb_l.wait_recv()
        yfar = []
        for q in range(DY_Q):
            c = far_cols(q)
            yfar.append((go(dyg.at[3, 0, lo, c], dyg.at[2, 0, lo, c], right, "yrr"),
                         go(dyg.at[1, 0, hi, c], dyg.at[2, 0, hi, c], left, "yll")))
    with jax.named_scope("up12"):
        up(1)
        up(2)
    with jax.named_scope("y_near_fwd"):
        yb_r.wait_recv()
        y_s3 = go(dyg.at[3, 0], dyg.at[3, 1], sib, "ys")
        ya_l.wait_recv()
        y_s1 = go(dyg.at[1, 0], dyg.at[1, 1], sib, "ys")
    with jax.named_scope("up34"):
        for e in range(3, n_exp):
            up(e)

    y_s2 = []

    def y_far_fwd(q):
        c = far_cols(q)
        for copy in yfar[q]:
            copy.wait_recv()
        y_s2.append(go(dyg.at[2, 0, :, c], dyg.at[2, 1, :, c], sib, "ys"))

    with jax.named_scope("y_near"):
        y_far_fwd(0)
        y_s3.wait_recv()
        gather_dy(3, full)
        y_s1.wait_recv()
        gather_dy(1, full)

    def down(e, q):
        c = dcol[q]
        val = lax.dot_general(dz[e, :, c], w2[e, :, c], NT, preferred_element_type=F32)
        if q > 0:
            val = val + dh[e]
        if q < DY_Q - 1:
            dh[e] = val
        else:
            da[e] = (val * bb[e].astype(F32) * qq[e]).astype(BF16)
            db[e] = (val * uu[e]).astype(BF16)

    w2copy.wait()
    for q in range(DY_Q):
        with jax.named_scope(f"y_far{q}"):
            if q + 1 < DY_Q:
                y_far_fwd(q + 1)
            y_s2[q].wait_recv()
            gather_dy(2, dcol[q])
        with jax.named_scope(f"down{q}"):
            for e in range(n_exp):
                down(e, q)

    qx = d // DX_Q
    sib_copies = []

    def dx_block(q):
        c = slice(q * qx, (q + 1) * qx)
        for e in range(n_exp):
            v = lax.dot_general(w1[e, c, :], da[e], NT, preferred_element_type=F32)
            v = v + lax.dot_general(w3[e, c, :], db[e], NT, preferred_element_type=F32)
            dxq[e] = jnp.transpose(v).astype(BF16)
        for s in range(n_chip):
            rows = dxq[:, s * rc_rows:(s + 1) * rc_rows, :].reshape(used, qx)
            part[q, s] = jnp.dot(pt[s, :, :used], rows, preferred_element_type=F32).reshape(2, tok, qx)
        sib_copies.append(go(part.at[q, :, 1], sibr.at[q], sib, "p%d" % q))

    def finish(q):
        c = slice(q * qx, (q + 1) * qx)
        sib_copies[q].wait_recv()

        def total(s, rs):
            return part[q, s, 0, rs] + sibr[q, s, rs]

        a, b = slice(0, half), slice(half, tok)
        r1[a, c] = total(2, a)
        r1[b, c] = total(1, b)
        l1[a, c] = total(3, a)
        l1[b, c] = total(2, b)
        ra[:, c] = total(1, a)
        lb[:, c] = total(3, b)
        own[:, c] = part[q, 0, 0] + sibr[q, 0]

    for q in range(DX_Q):
        with jax.named_scope(f"dx{q}"):
            dx_block(q)
        if q > 0:
            with jax.named_scope(f"finish{q - 1}"):
                finish(q - 1)
    with jax.named_scope(f"finish{DX_Q - 1}"):
        finish(DX_Q - 1)

    with jax.named_scope("send_wait"):
        whole = {"mr": mt.at[0], "ml": mt.at[0, 0], "ms": mt.at[:, 0]}
        for name, buf in (("x", xg), ("y", dyg)):
            whole.update({name + "r": buf.at[0, 0], name + "l": buf.at[0, 0], name + "s": buf.at[:, 0],
                          name + "rr": buf.at[0, 0, lo], name + "ll": buf.at[0, 0, hi]})
        for q in range(DX_Q):
            whole["p%d" % q] = part.at[q, :, 1]
        for i, group in enumerate(groups):
            describe(whole[group], whole[group], sib, i, 0).wait_send()
    assert (counter[0], len(groups)) == (N_COPIES, N_GROUPS)


def run_exchange(x, dy, ids, slots, gates, w1, w3, w2, n_dev, cap):
    n_exp, d, f = w1.shape
    tok = x.shape[0]
    half = tok // 2
    n_chip = n_dev // 2
    rows = n_dev * cap
    used = n_exp * 2 * cap
    qx = d // DX_Q
    any_spec = pl.BlockSpec(memory_space=pl.ANY)
    vmem_spec = pl.BlockSpec(memory_space=pltpu.VMEM)
    sds = OUT_TYPE
    outs = (
        sds((n_exp, rows, d), BF16), sds((n_exp, rows, d), BF16),
        sds((n_exp, rows, f), BF16), sds((n_exp, rows, f), BF16), sds((n_exp, rows, f), BF16),
        sds((tok, d), F32), sds((tok, d), F32), sds((half, d), F32), sds((half, d), F32), sds((tok, d), F32),
    )
    scratch = [
        pltpu.VMEM((n_chip, 2, tok, d), BF16),
        pltpu.VMEM((n_chip, 2, tok, d), BF16),
        pltpu.VMEM(ids.shape, jnp.int32),
        pltpu.VMEM(ids.shape, jnp.int32),
        pltpu.VMEM(ids.shape, F32),
        pltpu.VMEM((n_chip, 2, 16, 2 * tok), F32),
        pltpu.VMEM((n_exp, d, f), BF16),
        pltpu.VMEM((n_exp, d, f), BF16),
        pltpu.VMEM((n_exp, f, d), BF16),
        pltpu.VMEM((n_exp, rows, f), F32),
        pltpu.VMEM((n_exp, rows, f), F32),
        pltpu.VMEM((n_exp, rows, f), BF16),
        pltpu.VMEM((n_exp, rows, f), F32),
        pltpu.VMEM((n_exp, rows, qx), BF16),
        pltpu.VMEM((n_chip, KEY_STRIDE, 2 * tok), BF16),
        pltpu.VMEM((n_chip, 2 * tok, KEY_STRIDE), BF16),
        pltpu.VMEM((n_chip, KEY_STRIDE, 1), F32),
        pltpu.VMEM((DX_Q, n_chip, 2, tok, qx), F32),
        pltpu.VMEM((DX_Q, n_chip, tok, qx), F32),
        pltpu.SemaphoreType.DMA((5,)),
        pltpu.SemaphoreType.DMA((2 * n_exp + 1,)),
        pltpu.SemaphoreType.DMA((N_GROUPS,)),
        pltpu.SemaphoreType.DMA((N_COPIES,)),
    ]
    return pl.pallas_call(
        functools.partial(exchange_kernel, n_dev, cap),
        out_shape=outs,
        in_specs=[any_spec] * 8,
        out_specs=(vmem_spec,) * len(outs),
        scratch_shapes=scratch,
        compiler_params=pltpu.CompilerParams(
            collective_id=0, has_side_effects=True, vmem_limit_bytes=54_000_000),
        name="exchange",
    )(x, dy, ids, slots, gates, w1, w3, w2)


def grad_in_kernel(blk, x, da, db, g1_hbm, g3_hbm, g1, g3, sem):
    n_exp, rows, d = x.shape
    n_blk = d // blk

    def store(e, k):
        rs = pl.ds(k * blk, blk)
        return [pltpu.make_async_copy(src.at[e, rs], dst.at[e, rs], sem.at[o, e, k])
                for o, (src, dst) in enumerate(((g1, g1_hbm), (g3, g3_hbm)))]

    def step(e, carry):
        for k in range(n_blk):
            rs = slice(k * blk, (k + 1) * blk)
            xt = x[e, :, rs]
            g1[e, rs, :] = lax.dot_general(xt, da[e], TN, preferred_element_type=F32)
            g3[e, rs, :] = lax.dot_general(xt, db[e], TN, preferred_element_type=F32)
            for c in store(e, k):
                c.start()
        return carry

    lax.fori_loop(0, n_exp, step, 0)

    def drain(e, carry):
        for k in range(n_blk):
            for c in store(e, k):
                c.wait()
        return carry

    lax.fori_loop(0, n_exp, drain, 0)


def grad_in(xb, da, db, blk=512):
    n_exp, rows, d = xb.shape
    f = da.shape[2]
    any_spec = pl.BlockSpec(memory_space=pl.ANY)
    out = jax.ShapeDtypeStruct((n_exp, d, f), F32)
    return pl.pallas_call(
        functools.partial(grad_in_kernel, blk),
        out_shape=(out, out),
        in_specs=[pl.BlockSpec(memory_space=pltpu.VMEM)] * 3,
        out_specs=(any_spec, any_spec),
        scratch_shapes=[
            pltpu.VMEM(out.shape, F32), pltpu.VMEM(out.shape, F32),
            pltpu.SemaphoreType.DMA((2, n_exp, d // blk))],
        compiler_params=pltpu.CompilerParams(vmem_limit_bytes=40_000_000),
        cost_estimate=pl.CostEstimate(flops=4 * n_exp * rows * d * f, bytes_accessed=8 * n_exp * d * f, transcendentals=0),
        name="grad_in",
    )(xb, da, db)


def grad_out_kernel(blk, h, dz, g_hbm, g, sem):
    n_exp, rows, f = h.shape
    n_blk = f // blk

    def store(e, k):
        rs = pl.ds(k * blk, blk)
        return pltpu.make_async_copy(g.at[e, rs], g_hbm.at[e, rs], sem.at[e, k])

    def step(e, carry):
        for k in range(n_blk):
            rs = slice(k * blk, (k + 1) * blk)
            g[e, rs, :] = lax.dot_general(h[e, :, rs], dz[e], TN, preferred_element_type=F32)
            store(e, k).start()
        return carry

    lax.fori_loop(0, n_exp, step, 0)

    def drain(e, carry):
        for k in range(n_blk):
            store(e, k).wait()
        return carry

    lax.fori_loop(0, n_exp, drain, 0)


def grad_out(h, dz, blk=256):
    n_exp, rows, f = h.shape
    d = dz.shape[2]
    out = jax.ShapeDtypeStruct((n_exp, f, d), F32)
    return pl.pallas_call(
        functools.partial(grad_out_kernel, blk),
        out_shape=out,
        in_specs=[pl.BlockSpec(memory_space=pltpu.VMEM)] * 2,
        out_specs=pl.BlockSpec(memory_space=pl.ANY),
        scratch_shapes=[pltpu.VMEM(out.shape, F32), pltpu.SemaphoreType.DMA((n_exp, f // blk))],
        compiler_params=pltpu.CompilerParams(vmem_limit_bytes=24_000_000),
        cost_estimate=pl.CostEstimate(flops=2 * n_exp * rows * d * f, bytes_accessed=4 * n_exp * d * f, transcendentals=0),
        name="grad_out",
    )(h, dz)


def combine_kernel(own, r1, l1, r2, l2, out):
    half = r2.shape[0]
    out[:half, :] = (own[:half, :] + l1[:half, :] + r2[...]).astype(BF16)
    out[half:, :] = (own[half:, :] + r1[half:, :] + l2[...]).astype(BF16)


def combine(own, r1, l1, r2, l2):
    return pl.pallas_call(
        combine_kernel,
        out_shape=jax.ShapeDtypeStruct(own.shape, BF16),
        in_specs=[pl.BlockSpec(memory_space=pltpu.VMEM)] * 5,
        out_specs=pl.BlockSpec(memory_space=pltpu.VMEM),
        compiler_params=pltpu.CompilerParams(vmem_limit_bytes=8_000_000),
        name="combine",
    )(own, r1, l1, r2, l2)


def solution(mesh):
    n_dev = mesh.shape["ep"]
    n_chip = n_dev // 2

    def local_step(x_loc, dy_loc, ids_loc, gate_loc, slot_loc, w_gate, w_down, w_up):
        tok, top_k = ids_loc.shape
        n_local = w_gate.shape[0]
        cap = slot_capacity(tok, top_k, n_local * n_dev)
        half = tok // 2
        xb, dz, h, da, db, r1, l1, ra, lb, own = run_exchange(
            x_loc, dy_loc, ids_loc.T, slot_loc.T, gate_loc.T, w_gate, w_up, w_down, n_dev, cap)
        to_right = [(c * 2 + k, (c + 1) % n_chip * 2 + k) for c in range(n_chip) for k in range(2)]
        to_left = [(b, a) for a, b in to_right]
        r1 = lax.ppermute(r1, "ep", to_right)
        l1 = lax.ppermute(l1, "ep", to_left)
        g_gate, g_up = grad_in(xb, da, db)
        g_gate, g_up, r1, l1 = lax.optimization_barrier((g_gate, g_up, r1, l1))
        r2 = lax.ppermute(ra + r1[:half], "ep", to_right)
        l2 = lax.ppermute(lb + l1[half:], "ep", to_left)
        g_down = grad_out(h, dz)
        dx = combine(own, r1, l1, r2, l2)
        return dx, g_gate, g_down, g_up

    tok_spec = P(("dp", "ep"), None)
    w_spec = P("ep", None, None)
    grad_spec = P(("dp", "ep"), None, None)
    return jax.shard_map(
        local_step, mesh=mesh,
        in_specs=(tok_spec,) * 5 + (w_spec,) * 3,
        out_specs=(tok_spec, grad_spec, grad_spec, grad_spec),
        check_vma=False)
```
